32 devices in a mesh: gx: 4 (over z), gy: 4 (over y, x), gz: 2 (over core).
Axes of the slice: x: 2, y: 2, z: 4, core: 2. Of those that a mesh axis runs over, the one named last changes fastest.
Arguments:
- log_range: float32 [32, 128, 512], P('gz', 'gx', 'gy'), may hold values from -0.5 to 1.5
- sea_mask: int32 [32, 128, 512], P('gz', 'gx', 'gy'), may hold values 0 or 1
- forcing: float32 [32, 128, 512], P('gz', 'gx', 'gy'), may hold values from -24 to 24
- cotangent: float32 [32, 128, 512], P('gz', 'gx', 'gy'), may hold values from -24 to 24
Outputs:
- iterate: float32 [32, 128, 512], P('gz', 'gx', 'gy')
- range_grad: float32 [32, 128, 512], P('gz', 'gx', 'gy')
The draws below stay inside these ranges and needn't reach their ends.
All inputs are finite; a program needn't handle non-finite values. No bound on the sum of `sea_mask` on one device may be relied on, other than what follows from the above.
Results may differ from the reference program's by a relative error of at most 0.00002.
Values sent between devices are 32-bit elements; how exact they have to be, the bound alone decides.
No kernel may reach another device: no remote copies, remote signals or barrier semaphores. Data moves between devices by JAX's collectives and lax.ppermute only.
A program may use at most 64 MiB of HBM per device.

```python
import jax
import jax.numpy as jnp

SWEEPS = 4
NZ = 32
NX = 128
NY = 512


def plant(drawn, own_key, smallest, largest):
    longest = drawn.shape.index(max(drawn.shape))
    spots = []
    for shift in (0, 1):
        where = [jax.random.randint(jax.random.fold_in(own_key, axis), (), 0, length) for axis, length in enumerate(drawn.shape)]
        where[longest] = (where[longest] + shift) % drawn.shape[longest]
        spots.append(tuple(where))
    return drawn.at[spots[0]].set(smallest).at[spots[1]].set(largest)


def steps_of(key, dims, cuts, least, top_value):
    gain, own = 1.0, jax.random.fold_in(key, 6)
    for axis_at, parts in cuts:
        heights = jnp.exp(jax.random.uniform(jax.random.fold_in(own, axis_at), (parts,), jnp.float32, least / len(cuts), top_value / len(cuts)))
        gain = gain * jnp.repeat(heights, dims[axis_at] // parts).reshape([-1 if axis == axis_at else 1 for axis in range(len(dims))])
    return gain


def normal_values(own_key, shape, deviation, limit, shards=(), dtype=jnp.bfloat16):
    entries = deviation * jax.random.normal(own_key, shape, jnp.float32)
    if shards:
        entries = entries * steps_of(own_key, shape, shards, -0.22, 0.18)
    return jnp.clip(entries, -limit, limit).astype(dtype)


def setup_inputs(seed: int = 0) -> dict:
    arg_keys = jax.random.split(jax.random.key(seed), 5)
    return {
        "log_range": jnp.clip(-0.5 + 2.0 * jax.random.uniform(arg_keys[0], (NZ, NX, NY), jnp.float32) ** steps_of(arg_keys[0], (NZ, NX, NY), ((0, 2), (1, 4), (2, 4)), -0.2, 0.2), -0.5, 1.5),
        "sea_mask": plant((jax.random.randint(arg_keys[1], (NZ, NX, NY), 0, 4) < 3).astype(jnp.int32), jax.random.fold_in(arg_keys[1], 1), 0, 1),
        "forcing": normal_values(arg_keys[2], (NZ, NX, NY), 4.0, 24.0, ((0, 2), (1, 4), (2, 4)), jnp.float32),
        "cotangent": normal_values(arg_keys[3], (NZ, NX, NY), 4.0, 24.0, ((0, 2), (1, 4), (2, 4)), jnp.float32),
    }


relaxation = 0.9

def neighbours(field):
    padded = jnp.pad(field, 1)
    total = padded[2:, 1:-1, 1:-1] + padded[:-2, 1:-1, 1:-1]
    total = total + padded[1:-1, 2:, 1:-1] + padded[1:-1, :-2, 1:-1]
    total = total + padded[1:-1, 1:-1, 2:] + padded[1:-1, 1:-1, :-2]
    return total

def reference(log_range, sea_mask, forcing, cotangent):
    sea = sea_mask.astype(jnp.float32)

    def sweeps(values):
        diagonal = sea * (6.0 + jnp.exp(-2.0 * values)) + (1.0 - sea)
        state = jnp.zeros_like(forcing)
        for step in range(SWEEPS):
            state = (1.0 - relaxation) * state + relaxation * (forcing + sea * neighbours(sea * state)) / diagonal
        return state
    iterate, pullback = jax.vjp(sweeps, log_range)
    range_grad = pullback(cotangent)[0]
    return (iterate, range_grad)
```

```python
import functools

import jax
import jax.numpy as jnp
from jax import lax
from jax.experimental import pallas as pl
from jax.experimental.pallas import tpu as pltpu
from jax.sharding import PartitionSpec as P

SWEEPS = 4
RELAX = 0.9
KEEP = 1.0 - RELAX
SUB, LANES, DEPTH, GROUP = 8, 128, SWEEPS - 1, 6
AXES = ("gx", "gy", "gz")
ALL = slice(None)


def pair_swaps(sizes, axis, parity):
    nx, ny, nz = sizes
    pairs = []
    for i in range(nx):
        for j in range(ny):
            for k in range(nz):
                to = [i, j, k]
                other = to[axis] + (1 if to[axis] % 2 == parity else -1)
                if 0 <= other < sizes[axis]:
                    to[axis] = other
                else:
                    to[2] = 1 - k
                pairs.append(((i * ny + j) * nz + k, (to[0] * ny + to[1]) * nz + to[2]))
    return pairs


def iota(dim):
    return lax.broadcasted_iota(jnp.int32, (SUB, LANES), dim)


def level(t, lz):
    return jnp.where(lax.axis_index("gz") == 0, lz - 1 - t, t)


def prepare_kernel(lr, sea, src, cot, c_out, b_out, h_out, e_out, land_out, z_out):
    lz, lx, _ = lr.shape
    for t in range(lz):
        z = level(t, lz)
        for r in range(0, lx, SUB):
            rows = slice(r, r + SUB)
            wet = sea[z, rows, :] != 0
            decay = jnp.exp(-2.0 * lr[z, rows, :])
            c = jnp.where(wet, RELAX / (6.0 + decay), 0.0)
            f = src[z, rows, :]
            b = c * f
            h = c * cot[z, rows, :]
            c_out[t, rows, :] = c
            b_out[t, rows, :] = b
            h_out[t, rows, :] = h
            e_out[t, rows, :] = jnp.where(wet, (2.0 / RELAX) * decay, 0.0)
            land_out[t, rows, :] = jnp.where(
                wet, 0.0, RELAX * (1.0 + KEEP + KEEP**2 + KEEP**3) * f
            )
            if t < DEPTH:
                z_out[t, rows, :] = b
                z_out[DEPTH + t, rows, :] = h
            if t < DEPTH - 1:
                z_out[2 * DEPTH + t, rows, :] = c


def local_or_z(local, zin, base, depth, z):
    if z >= DEPTH:
        return local, z - DEPTH
    t = DEPTH - 1 - z
    return (zin, base + t) if t < depth else (None, 0)


def pack_x_kernel(c_in, b_in, h_in, zin, a_out, b_out):
    lz, lx, _ = c_in.shape
    odd = lax.axis_index("gx") % 2 == 1
    row = iota(0)
    for z in range(lz + DEPTH):
        faces = []
        for rows, s in ((slice(0, SUB), 1), (slice(lx - SUB, lx), -1)):
            br, bi = local_or_z(b_in, zin, 0, DEPTH, z)
            hr, hi = local_or_z(h_in, zin, DEPTH, DEPTH, z)
            cr, ci = local_or_z(c_in, zin, 2 * DEPTH, DEPTH - 1, z)
            b = br[bi, rows, :]
            h = hr[hi, rows, :]
            h = pltpu.roll(h, (s * DEPTH) % SUB, 0)
            if cr is None:
                c = jnp.zeros_like(b)
            else:
                c = pltpu.roll(cr[ci, rows, :], (s * 2 * DEPTH) % SUB, 0)
            at = row if s == 1 else SUB - 1 - row
            faces.append(jnp.where(at < DEPTH, b, jnp.where(at < 2 * DEPTH, h, c)))
        low, high = faces
        a_out[z] = jnp.where(odd, low, high)
        b_out[z] = jnp.where(odd, high, low)


def x_halo(a_in, b_in, z, index, size, row):
    odd = index % 2 == 1
    zero = jnp.zeros((SUB, LANES), jnp.float32)
    before = jnp.where(index > 0, jnp.where(odd, a_in[z], b_in[z]), zero)
    after = jnp.where(index < size - 1, jnp.where(odd, b_in[z], a_in[z]), zero)
    up = SUB - 1 - row

    def merge(depth, shift):
        lo = pltpu.roll(before, shift, 0) if shift else before
        hi = pltpu.roll(after, SUB - shift, 0) if shift else after
        return jnp.where(row < depth, hi, jnp.where(up < depth, lo, 0.0))

    return merge(DEPTH, 0), merge(DEPTH, DEPTH), merge(DEPTH - 1, 2 * DEPTH)


def place_of(lane, lz):
    group = lane // GROUP
    inside = group < lz + DEPTH - 1
    return jnp.where(inside, lane - GROUP * group, -1), jnp.where(inside, group, -1)


def turn(g):
    return (GROUP * g + DEPTH) % LANES


def pack_y_kernel(nx, c_in, b_in, h_in, zin, xa, xb, cm, bm, hm, pb_out, ph_out, ya, yb):
    lz, lx, _ = c_in.shape
    ix, iy = lax.axis_index("gx"), lax.axis_index("gy")
    row, lane = iota(0), iota(1)
    place, group = place_of(lane, lz)
    zero = jnp.zeros((SUB, LANES), jnp.float32)
    tiles = lx // SUB + 1
    halo = slice(SUB * tiles, SUB * (tiles + 1))
    acc = [[zero] * tiles for _ in range(3)]
    for z in range(lz + DEPTH):
        parts = x_halo(xa, xb, z, ix, nx, row)
        local = (
            local_or_z(b_in, zin, 0, DEPTH, z),
            local_or_z(h_in, zin, DEPTH, DEPTH, z),
            local_or_z(c_in, zin, 2 * DEPTH, DEPTH - 1, z),
        )
        for f, store in enumerate((bm, hm, cm)):
            ref, i = local[f]
            for t in range(tiles):
                if t == 0:
                    tile = parts[f]
                    store[z, halo, :] = tile
                else:
                    tile = zero if ref is None else ref[i, SUB * (t - 1) : SUB * t, :]
                store[z, SUB * t : SUB * (t + 1), :] = tile
                if z >= 1:
                    g = z - 1
                    acc[f][t] = jnp.where(
                        group == g, pltpu.roll(tile, turn(g), 1), acc[f][t]
                    )
    for store in (bm, hm, cm):
        for t in range(tiles + 1):
            store[lz + DEPTH, SUB * t : SUB * (t + 1), :] = zero
    odd = iy % 2 == 1
    for t in range(tiles):
        rows = slice(SUB * t, SUB * (t + 1))
        pb, ph, pc = acc[0][t], acc[1][t], acc[2][t]
        pb_out[rows, :] = pb
        ph_out[rows, :] = ph
        upper = jnp.where(place < DEPTH, pb, pltpu.roll(ph, DEPTH, 1))
        lower = jnp.where(place >= DEPTH, pb, pltpu.roll(ph, LANES - DEPTH, 1))
        ya[0, rows, :] = jnp.where(odd, lower, upper)
        yb[0, rows, :] = jnp.where(odd, upper, lower)
        ya[1, rows, :] = pc
        yb[1, rows, :] = pc


def sweep_kernel(
    ny, cm, bm, hm, pb, ph, ya, yb, e_in, land_in, it_out, rg_out,
    y1, y2, h1, h2, sb, sh, sc, sy1, sy2, sh1, sh2,
):
    lz, lx, _ = e_in.shape
    iy = lax.axis_index("gy")
    lane = iota(1)
    place, group = place_of(lane, lz)
    tiles = lx // SUB + 1
    halo = slice(SUB * tiles, SUB * (tiles + 1))
    zero = jnp.zeros((SUB, LANES), jnp.float32)
    first, last = lane == 0, lane == LANES - 1
    inner = (place == DEPTH - 1) | (place == DEPTH)
    in_group = jnp.where(inner, group, -1)
    below, above = place == DEPTH - 1, place == DEPTH
    odd = iy % 2 == 1

    def put(ref, t, value):
        ref[SUB * t : SUB * (t + 1), :] = value
        if t == 0:
            ref[halo, :] = value

    for t in range(tiles):
        rows = slice(SUB * t, SUB * (t + 1))
        got = []
        for k in range(2):
            a, b = ya[k, rows, :], yb[k, rows, :]
            got.append(
                (
                    jnp.where(iy > 0, jnp.where(odd, a, b), zero),
                    jnp.where(iy < ny - 1, jnp.where(odd, b, a), zero),
                )
            )
        (lo, hi), (lo_c, hi_c) = got
        near, far = (place >= 0) & (place < DEPTH), place >= DEPTH
        put(sb, t, jnp.where(near, lo, jnp.where(far, hi, 0.0)))
        put(
            sh, t,
            jnp.where(
                near, pltpu.roll(lo, LANES - DEPTH, 1),
                jnp.where(far, pltpu.roll(hi, DEPTH, 1), 0.0),
            ),
        )
        put(sc, t, jnp.where(near, lo_c, jnp.where(far, hi_c, 0.0)))

    def shifted(ref, t, pre=()):
        at = SUB * (tiles if t == 0 else t)
        minus = ref[pre + (slice(at - 1, at - 1 + SUB), ALL)]
        plus = ref[pre + (slice(SUB * t + 1, SUB * t + 1 + SUB), ALL)]
        return minus, plus

    def spread(v, strip, edge_tiles, z, t):
        rows = slice(SUB * t, SUB * (t + 1))
        here = v[z, rows, :]
        minus, plus = shifted(v, t, (z,))
        edge = pltpu.roll(edge_tiles[t], LANES - turn(z - 1), 1)
        left = pltpu.roll(jnp.where(last, edge, here), 1, 1)
        right = pltpu.roll(jnp.where(first, edge, here), LANES - 1, 1)
        return (v[z - 1, rows, :] + v[z + 1, rows, :]) + (minus + plus) + (left + right), here

    def strip_step(v, extra, source, out, ends):
        for t in range(tiles):
            rows = slice(SUB * t, SUB * (t + 1))
            here = v[rows, :]
            minus, plus = shifted(v, t)
            end = ends(t)
            near = pltpu.roll(jnp.where(above, end, here), LANES - 1, 1)
            far = pltpu.roll(jnp.where(below, end, here), 1, 1)
            total = (minus + plus) + (near + far)
            total = total + (pltpu.roll(here, GROUP, 1) + pltpu.roll(here, LANES - GROUP, 1))
            value = KEEP * here + sc[rows, :] * total
            if source is not None:
                value = value + source[rows, :]
            put(out, t, value)

    def step(v, strip, source, out, start, collect):
        ends = []
        edge_tiles = [strip[SUB * t : SUB * (t + 1), :] for t in range(tiles)]
        for t in range(tiles):
            rows = slice(SUB * t, SUB * (t + 1))
            end = zero
            for z in range(start, lz + DEPTH):
                total, here = spread(v, strip, edge_tiles, z, t)
                value = cm[z, rows, :] * total
                if source is not None:
                    value = source[z, rows, :] + value
                value = KEEP * here + value
                out[z, rows, :] = value
                if t == 0:
                    out[z, halo, :] = value
                if collect:
                    g = z - 1
                    end = jnp.where(in_group == g, pltpu.roll(value, turn(g), 1), end)
            ends.append(end)
        for ref in (out,):
            for t in range(tiles + 1):
                ref[lz + DEPTH, SUB * t : SUB * (t + 1), :] = zero
        return ends

    strip_step(sb, None, sb, sy1, lambda t: pb[SUB * t : SUB * (t + 1), :])
    strip_step(sh, None, None, sh1, lambda t: ph[SUB * t : SUB * (t + 1), :])
    ends_h = step(hm, sh, None, h1, 1, True)
    ends_y = step(bm, sb, bm, y1, 1, True)
    strip_step(sh1, None, None, sh2, lambda t: ends_h[t])
    strip_step(sy1, None, sb, sy2, lambda t: ends_y[t])
    step(h1, sh1, None, h2, 2, False)
    step(y1, sy1, bm, y2, 2, False)
    edge_h = [sh2[SUB * t : SUB * (t + 1), :] for t in range(tiles)]
    edge_y = [sy2[SUB * t : SUB * (t + 1), :] for t in range(tiles)]
    for t in range(1, tiles):
        rows, block = slice(SUB * t, SUB * (t + 1)), slice(SUB * (t - 1), SUB * t)
        for z in range(DEPTH, lz + DEPTH):
            k = z - DEPTH
            c, b = cm[z, rows, :], bm[z, rows, :]
            total_h, g2 = spread(h2, sh2, edge_h, z, t)
            total_y, x3 = spread(y2, sy2, edge_y, z, t)
            g1 = KEEP * g2 + c * total_h
            w3 = b + c * total_y
            x2 = y1[z, rows, :]
            w2 = x3 - KEEP * x2
            w1 = x2 - KEEP * b
            s = (g1 * b + g2 * w1) + (h1[z, rows, :] * w2 + hm[z, rows, :] * w3)
            out = level(k, lz)
            it_out[out, block, :] = (KEEP * x3 + w3) + land_in[k, block, :]
            rg_out[out, block, :] = e_in[k, block, :] * s


def body(nx, ny, log_range, sea_mask, forcing, cotangent):
    lz, lx, ly = forcing.shape
    f32 = jnp.float32
    sizes = (nx, ny, 2)
    vmem = pl.BlockSpec(memory_space=pltpu.VMEM)
    params = pltpu.CompilerParams(vmem_limit_bytes=32 * 2**20)

    def call(kernel, shapes, args, name, scratch=(), flops=1):
        return pl.pallas_call(
            kernel,
            out_shape=[jax.ShapeDtypeStruct(s, f32) for s in shapes],
            in_specs=[vmem] * len(args),
            out_specs=[vmem] * len(shapes),
            scratch_shapes=[pltpu.VMEM(s, f32) for s in scratch],
            compiler_params=params,
            cost_estimate=pl.CostEstimate(flops=flops, bytes_accessed=2**20, transcendentals=0),
            name=name,
        )(*args)

    block = (lz, lx, ly)
    store = (lz + DEPTH + 1, lx + 2 * SUB, ly)
    strip = (lx + 2 * SUB, LANES)
    packed = (lx + SUB, LANES)
    c, b, h, e, land, zmsg = call(
        prepare_kernel,
        [block] * 5 + [(3 * DEPTH - 1, lx, ly)],
        (log_range, sea_mask, forcing, cotangent),
        "prepare",
    )
    swap = [(d, d ^ 1) for d in range(2 * nx * ny)]
    zin = lax.ppermute(zmsg, AXES, swap)
    xa, xb = call(pack_x_kernel, [(lz + DEPTH, SUB, ly)] * 2, (c, b, h, zin), "pack_x")
    xa = lax.ppermute(xa, AXES, pair_swaps(sizes, 0, 0))
    xb = lax.ppermute(xb, AXES, pair_swaps(sizes, 0, 1))
    cm, bm, hm, pb, ph, ya, yb = call(
        functools.partial(pack_y_kernel, nx),
        [store] * 3 + [packed] * 2 + [(2,) + packed] * 2,
        (c, b, h, zin, xa, xb),
        "pack_y",
    )
    ya = lax.ppermute(ya, AXES, pair_swaps(sizes, 1, 0))
    yb = lax.ppermute(yb, AXES, pair_swaps(sizes, 1, 1))
    return call(
        functools.partial(sweep_kernel, ny),
        [block] * 2,
        (cm, bm, hm, pb, ph, ya, yb, e, land),
        "sweep",
        [store] * 4 + [strip] * 7,
    )


def solution(mesh):
    nx, ny = mesh.shape["gx"], mesh.shape["gy"]
    spec = P("gz", "gx", "gy")
    return jax.shard_map(
        lambda *args: tuple(body(nx, ny, *args)),
        mesh=mesh,
        in_specs=(spec,) * 4,
        out_specs=(spec,) * 2,
        check_vma=False,
    )
```

```python
import functools

import jax
import jax.numpy as jnp
from jax import lax
from jax.experimental import pallas as pl
from jax.experimental.pallas import tpu as pltpu
from jax.sharding import PartitionSpec as P

SWEEPS = 4
RELAX = 0.9
KEEP = 1.0 - RELAX
SUB, LANES, DEPTH = 8, 128, SWEEPS - 1
OWN = 2 * DEPTH
GROUP = 2 * (OWN + DEPTH)
STRIDE = 3
AXES = ("gx", "gy", "gz")
ALL = slice(None)


def pair_swaps(sizes, axis, parity):
    nx, ny, nz = sizes
    pairs = []
    for i in range(nx):
        for j in range(ny):
            for k in range(nz):
                to = [i, j, k]
                other = to[axis] + (1 if to[axis] % 2 == parity else -1)
                if 0 <= other < sizes[axis]:
                    to[axis] = other
                else:
                    to[2] = 1 - k
                pairs.append(((i * ny + j) * nz + k, (to[0] * ny + to[1]) * nz + to[2]))
    return pairs


def iota(dim):
    return lax.broadcasted_iota(jnp.int32, (SUB, LANES), dim)


def level(t, lz):
    return jnp.where(lax.axis_index("gz") == 0, lz - 1 - t, t)


def tile_rows(t):
    return slice(SUB * t, SUB * (t + 1))


def prepare_kernel(lr_h, sea_h, src_h, cot_h, c_out, b_out, h_out, e_out, land_out, z_out,
                   lr, sea, src, cot, sem):
    lz, lx, _ = lr.shape
    copies = [
        pltpu.make_async_copy(a, b, sem.at[i])
        for i, (a, b) in enumerate(((lr_h, lr), (sea_h, sea), (src_h, src), (cot_h, cot)))
    ]
    for copy in copies:
        copy.start()
    for copy in copies:
        copy.wait()
    for t in range(lz):
        z = level(t, lz)
        for r in range(0, lx, SUB):
            rows = slice(r, r + SUB)
            wet = sea[z, rows, :] != 0
            decay = jnp.exp(-2.0 * lr[z, rows, :])
            c = jnp.where(wet, RELAX / (6.0 + decay), 0.0)
            f = src[z, rows, :]
            b = c * f
            h = c * cot[z, rows, :]
            c_out[t, rows, :] = c
            b_out[t, rows, :] = b
            h_out[t, rows, :] = h
            e_out[t, rows, :] = jnp.where(wet, (2.0 / RELAX) * decay, 0.0)
            land_out[t, rows, :] = jnp.where(
                wet, 0.0, RELAX * (1.0 + KEEP + KEEP**2 + KEEP**3) * f
            )
            if t < DEPTH:
                z_out[t, rows, :] = b
                z_out[DEPTH + t, rows, :] = h
            if t < DEPTH - 1:
                z_out[2 * DEPTH + t, rows, :] = c


def local_or_z(local, zin, base, depth, z):
    if z >= DEPTH:
        return local, z - DEPTH
    t = DEPTH - 1 - z
    return (zin, base + t) if t < depth else (None, 0)


def pack_x_kernel(c_in, b_in, h_in, zin, a_out, b_out):
    lz, lx, _ = c_in.shape
    odd = lax.axis_index("gx") % 2 == 1
    row = iota(0)
    for z in range(lz + DEPTH):
        faces = []
        for rows, s in ((slice(0, SUB), 1), (slice(lx - SUB, lx), -1)):
            br, bi = local_or_z(b_in, zin, 0, DEPTH, z)
            hr, hi = local_or_z(h_in, zin, DEPTH, DEPTH, z)
            cr, ci = local_or_z(c_in, zin, 2 * DEPTH, DEPTH - 1, z)
            b = br[bi, rows, :]
            h = hr[hi, rows, :]
            h = pltpu.roll(h, (s * DEPTH) % SUB, 0)
            if cr is None:
                c = jnp.zeros_like(b)
            else:
                c = pltpu.roll(cr[ci, rows, :], (s * 2 * DEPTH) % SUB, 0)
            at = row if s == 1 else SUB - 1 - row
            faces.append(jnp.where(at < DEPTH, b, jnp.where(at < 2 * DEPTH, h, c)))
        low, high = faces
        a_out[z] = jnp.where(odd, low, high)
        b_out[z] = jnp.where(odd, high, low)


def x_halo(a_in, b_in, z, index, size, row):
    odd = index % 2 == 1
    zero = jnp.zeros((SUB, LANES), jnp.float32)
    before = jnp.where(index > 0, jnp.where(odd, a_in[z], b_in[z]), zero)
    after = jnp.where(index < size - 1, jnp.where(odd, b_in[z], a_in[z]), zero)
    up = SUB - 1 - row

    def merge(depth, shift):
        lo = pltpu.roll(before, shift, 0) if shift else before
        hi = pltpu.roll(after, SUB - shift, 0) if shift else after
        return jnp.where(row < depth, hi, jnp.where(up < depth, lo, 0.0))

    return merge(DEPTH, 0), merge(DEPTH, DEPTH), merge(DEPTH - 1, 2 * DEPTH)


def packed_place(lane, lz):
    group = lane // GROUP
    inside = group < -(-(lz + DEPTH) // STRIDE)
    return jnp.where(inside, group, -1), jnp.where(inside, lane - GROUP * group, -1)


def pack_y_kernel(nx, c_in, b_in, h_in, zin, xa, xb, cm, bm, hm, pc_out, pb_out, ph_out, ya, yb):
    lz, lx, _ = c_in.shape
    ix, iy = lax.axis_index("gx"), lax.axis_index("gy")
    row, lane = iota(0), iota(1)
    group, place = packed_place(lane, lz)
    zero = jnp.zeros((SUB, LANES), jnp.float32)
    tiles = lx // SUB + 1
    halo = tile_rows(tiles)
    acc = [[[zero] * tiles for _ in range(STRIDE)] for _ in range(3)]
    raw = jnp.where(place < 2 * OWN, group, -1)
    for z in range(lz + DEPTH):
        parts = x_halo(xa, xb, z, ix, nx, row)
        local = (
            local_or_z(c_in, zin, 2 * DEPTH, DEPTH - 1, z),
            local_or_z(b_in, zin, 0, DEPTH, z),
            local_or_z(h_in, zin, DEPTH, DEPTH, z),
        )
        for f, store in enumerate((cm, bm, hm)):
            ref, i = local[f]
            for t in range(tiles):
                if t == 0:
                    tile = parts[(f + 2) % 3]
                    store[z, halo, :] = tile
                else:
                    tile = zero if ref is None else ref[i, tile_rows(t - 1), :]
                store[z, tile_rows(t), :] = tile
                if f or z:
                    g, v = z // STRIDE, z % STRIDE
                    acc[f][v][t] = jnp.where(
                        raw == g, pltpu.roll(tile, (GROUP * g + OWN) % LANES, 1), acc[f][v][t]
                    )
    for store in (cm, bm, hm):
        for t in range(tiles + 1):
            store[lz + DEPTH, tile_rows(t), :] = zero
    odd = iy % 2 == 1
    for v in range(STRIDE):
        for t in range(tiles):
            rows = tile_rows(t)
            own = []
            for f in range(3):
                a = acc[f][v][t]
                moved = pltpu.roll(a, GROUP - 2 * OWN, 1)
                own.append(
                    jnp.where(place < OWN, a, jnp.where(place >= GROUP - OWN, moved, 0.0))
                )
            for ref, a in zip((pc_out, pb_out, ph_out), own):
                ref[v, rows, :] = a
            c, b, h = (acc[f][v][t] for f in range(3))
            first, last = OWN, DEPTH
            upper = jnp.where(
                place < DEPTH, pltpu.roll(b, LANES - last, 1),
                jnp.where(place < 2 * DEPTH, h, pltpu.roll(c, 2 * DEPTH - last, 1)),
            )
            lower = jnp.where(
                place < DEPTH, pltpu.roll(b, LANES - first, 1),
                jnp.where(place < 2 * DEPTH, pltpu.roll(h, LANES + DEPTH - first, 1), c),
            )
            ya[v, rows, :] = jnp.where(odd, lower, upper)
            yb[v, rows, :] = jnp.where(odd, upper, lower)


def main_kernel(cm, bm, hm, it_out, s_out, y1, y2, h1, h2):
    lz, lx, _ = it_out.shape
    tiles = lx // SUB + 1
    halo = tile_rows(tiles)
    zero = jnp.zeros((SUB, LANES), jnp.float32)

    def spread(v, z, t):
        rows = tile_rows(t)
        here = v[z, rows, :]
        at = SUB * (tiles if t == 0 else t) - 1
        total = v[z, at : at + SUB, :] + v[z, SUB * t + 1 : SUB * t + 1 + SUB, :]
        total = total + (v[z - 1, rows, :] + v[z + 1, rows, :])
        sides = pltpu.roll(here, 1, 1) + pltpu.roll(here, LANES - 1, 1)
        return total + sides, here

    def step(v, source, out, start):
        for z in range(start, lz + DEPTH):
            for t in range(tiles):
                rows = tile_rows(t)
                total, here = spread(v, z, t)
                value = cm[z, rows, :] * total
                if source is not None:
                    value = source[z, rows, :] + value
                value = KEEP * here + value
                out[z, rows, :] = value
                if t == 0:
                    out[z, halo, :] = value
        for t in range(tiles + 1):
            out[lz + DEPTH, tile_rows(t), :] = zero

    step(hm, None, h1, 1)
    step(bm, bm, y1, 1)
    step(h1, None, h2, 2)
    step(y1, bm, y2, 2)
    for z in range(DEPTH, lz + DEPTH):
        for t in range(1, tiles):
            rows, block = tile_rows(t), tile_rows(t - 1)
            k = z - DEPTH
            c, b = cm[z, rows, :], bm[z, rows, :]
            total_h, g2 = spread(h2, z, t)
            total_y, x3 = spread(y2, z, t)
            x2 = y1[z, rows, :]
            g1 = KEEP * g2 + c * total_h
            w3 = b + c * total_y
            it_out[k, block, :] = KEEP * x3 + w3
            s_out[k, block, :] = (g1 * b + g2 * (x2 - KEEP * b)) + (
                h1[z, rows, :] * (x3 - KEEP * x2) + hm[z, rows, :] * w3
            )


def edge_kernel(ny, pc, pb, ph, ya, yb, it_in, s_in, e_in, land_in, it_hbm, rg_hbm,
                cs, bs, hs, y1, y2, h1, h2, it_out, rg_out, sem):
    lz, lx, _ = e_in.shape
    iy = lax.axis_index("gy")
    lane = iota(1)
    group, place = packed_place(lane, lz)
    tiles = lx // SUB + 1
    halo = tile_rows(tiles)
    zero = jnp.zeros((SUB, LANES), jnp.float32)
    odd = iy % 2 == 1
    after = (place >= OWN) & (place < OWN + DEPTH)
    before = (place >= OWN + DEPTH) & (place < OWN + 2 * DEPTH)

    def put(ref, v, t, value):
        ref[v, tile_rows(t), :] = value
        if t == 0:
            ref[v, halo, :] = value

    for v in range(STRIDE):
        for t in range(tiles):
            rows = tile_rows(t)
            a, b = ya[v, rows, :], yb[v, rows, :]
            lo = jnp.where(iy > 0, jnp.where(odd, a, b), zero)
            hi = jnp.where(iy < ny - 1, jnp.where(odd, b, a), zero)
            for k, (ref, own) in enumerate(((bs, pb), (hs, ph), (cs, pc))):
                from_lo = pltpu.roll(lo, (OWN + DEPTH - k * DEPTH) % LANES, 1)
                from_hi = pltpu.roll(hi, (OWN - k * DEPTH) % LANES, 1) if k != 2 else hi
                put(ref, v, t,
                    jnp.where(before, from_lo, jnp.where(after, from_hi, own[v, rows, :])))

    def spread(ref, v, t):
        rows = tile_rows(t)
        here = ref[v, rows, :]
        at = SUB * (tiles if t == 0 else t) - 1
        total = ref[v, at : at + SUB, :] + ref[v, SUB * t + 1 : SUB * t + 1 + SUB, :]
        down = ref[(v - 1) % STRIDE, rows, :]
        up = ref[(v + 1) % STRIDE, rows, :]
        if v == 0:
            down = pltpu.roll(down, GROUP, 1)
        if v == STRIDE - 1:
            up = pltpu.roll(up, LANES - GROUP, 1)
        sides = pltpu.roll(here, 1, 1) + pltpu.roll(here, LANES - 1, 1)
        return total + (down + up) + sides, here

    def step(src, source, out):
        for v in range(STRIDE):
            for t in range(tiles):
                rows = tile_rows(t)
                total, here = spread(src, v, t)
                value = cs[v, rows, :] * total
                if source is not None:
                    value = source[v, rows, :] + value
                put(out, v, t, KEEP * here + value)

    step(hs, None, h1)
    step(bs, bs, y1)
    step(h1, None, h2)
    step(y1, bs, y2)
    its, ss = {}, {}
    for v in range(STRIDE):
        for t in range(1, tiles):
            rows = tile_rows(t)
            c, b = cs[v, rows, :], bs[v, rows, :]
            total_h, g2 = spread(h2, v, t)
            total_y, x3 = spread(y2, v, t)
            x2 = y1[v, rows, :]
            g1 = KEEP * g2 + c * total_h
            w3 = b + c * total_y
            it = KEEP * x3 + w3
            s = (g1 * b + g2 * (x2 - KEEP * b)) + (
                h1[v, rows, :] * (x3 - KEEP * x2) + hs[v, rows, :] * w3
            )
            its[v, t] = jnp.where(place < OWN, it, pltpu.roll(it, LANES - OWN, 1))
            ss[v, t] = jnp.where(place < OWN, s, pltpu.roll(s, LANES - OWN, 1))
    rim = (lane < DEPTH) | (lane >= LANES - DEPTH)
    copies = []
    for k in range(lz):
        z = level(k, lz)
        g, v = (k + DEPTH) // STRIDE, (k + DEPTH) % STRIDE
        shift = (LANES - DEPTH - (GROUP * g + DEPTH)) % LANES
        for t in range(1, tiles):
            block = tile_rows(t - 1)
            it = jnp.where(rim, pltpu.roll(its[v, t], shift, 1), it_in[k, block, :])
            s = jnp.where(rim, pltpu.roll(ss[v, t], shift, 1), s_in[k, block, :])
            it_out[k, block, :] = it + land_in[k, block, :]
            rg_out[k, block, :] = e_in[k, block, :] * s
        for i, (a, b) in enumerate(((it_out, it_hbm), (rg_out, rg_hbm))):
            copies.append(pltpu.make_async_copy(a.at[k], b.at[z], sem.at[i, k]))
            copies[-1].start()
    for copy in copies:
        copy.wait()


def body(nx, ny, log_range, sea_mask, forcing, cotangent):
    lz, lx, ly = forcing.shape
    f32 = jnp.float32
    sizes = (nx, ny, 2)
    vmem = pl.BlockSpec(memory_space=pltpu.VMEM)
    hbm = pl.BlockSpec(memory_space=pltpu.HBM)

    def call(kernel, shapes, args, name, scratch=(), flops=10**6, ins=vmem, outs=vmem):
        return pl.pallas_call(
            kernel,
            out_shape=[jax.ShapeDtypeStruct(s, f32) for s in shapes],
            in_specs=[ins] * len(args),
            out_specs=[outs] * len(shapes),
            scratch_shapes=[pltpu.VMEM(s, f32) if isinstance(s, tuple) else s for s in scratch],
            compiler_params=pltpu.CompilerParams(vmem_limit_bytes=16 * 2**20),
            cost_estimate=pl.CostEstimate(flops=flops, bytes_accessed=2**20, transcendentals=0),
            name=name,
        )(*args)

    block = (lz, lx, ly)
    store = (lz + DEPTH + 1, lx + 2 * SUB, ly)
    strip = (STRIDE, lx + 2 * SUB, LANES)
    packed = (STRIDE, lx + SUB, LANES)
    c, b, h, e, land, zmsg = call(
        prepare_kernel,
        [block] * 5 + [(3 * DEPTH - 1, lx, ly)],
        [
            pltpu.with_memory_space_constraint(a, pltpu.HBM)
            for a in (log_range, sea_mask, forcing, cotangent)
        ],
        "prepare",
        [block, pltpu.VMEM(block, jnp.int32), block, block, pltpu.SemaphoreType.DMA((4,))],
        ins=hbm,
    )
    swap = [(d, d ^ 1) for d in range(2 * nx * ny)]
    zin = lax.ppermute(zmsg, AXES, swap)
    xa, xb = call(pack_x_kernel, [(lz + DEPTH, SUB, ly)] * 2, (c, b, h, zin), "pack_x")
    xa = lax.ppermute(xa, AXES, pair_swaps(sizes, 0, 0))
    xb = lax.ppermute(xb, AXES, pair_swaps(sizes, 0, 1))
    cm, bm, hm, pc, pb, ph, ya, yb = call(
        functools.partial(pack_y_kernel, nx),
        [store] * 3 + [packed] * 5,
        (c, b, h, zin, xa, xb),
        "pack_y",
    )
    ya = lax.ppermute(ya, AXES, pair_swaps(sizes, 1, 0))
    yb = lax.ppermute(yb, AXES, pair_swaps(sizes, 1, 1))
    it, s = call(
        main_kernel, [block] * 2, (cm, bm, hm), "main", [store] * 4, flops=2 * 10**8
    )
    return call(
        functools.partial(edge_kernel, ny),
        [block] * 2,
        (pc, pb, ph, ya, yb, it, s, e, land),
        "edge",
        [strip] * 7 + [block] * 2 + [pltpu.SemaphoreType.DMA((2, lz))],
        outs=hbm,
    )


def solution(mesh):
    nx, ny = mesh.shape["gx"], mesh.shape["gy"]
    spec = P("gz", "gx", "gy")
    return jax.shard_map(
        lambda *args: tuple(body(nx, ny, *args)),
        mesh=mesh,
        in_specs=(spec,) * 4,
        out_specs=(spec,) * 2,
        check_vma=False,
    )
```

```python
import functools

import jax
import jax.numpy as jnp
from jax import lax
from jax.experimental import pallas as pl
from jax.experimental.pallas import tpu as pltpu
from jax.sharding import PartitionSpec as P

SWEEPS = 4
RELAX = 0.9
KEEP = 1.0 - RELAX
SUB, LANES, DEPTH = 8, 128, SWEEPS - 1
OWN = 2 * DEPTH
GROUP = 2 * (OWN + DEPTH)
STRIDE = 3
AXES = ("gx", "gy", "gz")
ALL = slice(None)


def pair_swaps(sizes, axis, parity):
    nx, ny, nz = sizes
    pairs = []
    for i in range(nx):
        for j in range(ny):
            for k in range(nz):
                to = [i, j, k]
                other = to[axis] + (1 if to[axis] % 2 == parity else -1)
                if 0 <= other < sizes[axis]:
                    to[axis] = other
                else:
                    to[2] = 1 - k
                pairs.append(((i * ny + j) * nz + k, (to[0] * ny + to[1]) * nz + to[2]))
    return pairs


def iota(dim):
    return lax.broadcasted_iota(jnp.int32, (SUB, LANES), dim)


def level(t, lz):
    return jnp.where(lax.axis_index("gz") == 0, lz - 1 - t, t)


def tile_rows(t):
    return slice(SUB * t, SUB * (t + 1))


def prepare_kernel(lr_h, sea_h, src_h, cot_h, c_out, b_out, h_out, e_out, land_out, z_out,
                   lr, sea, src, cot, sem):
    lz, lx, _ = lr.shape
    copies = [
        pltpu.make_async_copy(a, b, sem.at[i])
        for i, (a, b) in enumerate(((lr_h, lr), (sea_h, sea), (src_h, src), (cot_h, cot)))
    ]
    for copy in copies:
        copy.start()
    for copy in copies:
        copy.wait()
    for t in range(lz):
        z = level(t, lz)
        for r in range(0, lx, SUB):
            rows = slice(r, r + SUB)
            wet = sea[z, rows, :] != 0
            decay = jnp.exp(-2.0 * lr[z, rows, :])
            c = jnp.where(wet, RELAX / (6.0 + decay), 0.0)
            f = src[z, rows, :]
            b = c * f
            h = c * cot[z, rows, :]
            c_out[t, rows, :] = c
            b_out[t, rows, :] = b
            h_out[t, rows, :] = h
            e_out[t, rows, :] = jnp.where(wet, (2.0 / RELAX) * decay, 0.0)
            land_out[t, rows, :] = jnp.where(
                wet, 0.0, RELAX * (1.0 + KEEP + KEEP**2 + KEEP**3) * f
            )
            if t < DEPTH:
                z_out[t, rows, :] = b
                z_out[DEPTH + t, rows, :] = h
            if t < DEPTH - 1:
                z_out[2 * DEPTH + t, rows, :] = c


def local_or_z(local, zin, base, depth, z):
    if z >= DEPTH:
        return local, z - DEPTH
    t = DEPTH - 1 - z
    return (zin, base + t) if t < depth else (None, 0)


def pack_x_kernel(c_in, b_in, h_in, zin, a_out, b_out):
    lz, lx, _ = c_in.shape
    odd = lax.axis_index("gx") % 2 == 1
    row = iota(0)
    for z in range(lz + DEPTH):
        faces = []
        for rows, s in ((slice(0, SUB), 1), (slice(lx - SUB, lx), -1)):
            br, bi = local_or_z(b_in, zin, 0, DEPTH, z)
            hr, hi = local_or_z(h_in, zin, DEPTH, DEPTH, z)
            cr, ci = local_or_z(c_in, zin, 2 * DEPTH, DEPTH - 1, z)
            b = br[bi, rows, :]
            h = hr[hi, rows, :]
            h = pltpu.roll(h, (s * DEPTH) % SUB, 0)
            if cr is None:
                c = jnp.zeros_like(b)
            else:
                c = pltpu.roll(cr[ci, rows, :], (s * 2 * DEPTH) % SUB, 0)
            at = row if s == 1 else SUB - 1 - row
            faces.append(jnp.where(at < DEPTH, b, jnp.where(at < 2 * DEPTH, h, c)))
        low, high = faces
        a_out[z] = jnp.where(odd, low, high)
        b_out[z] = jnp.where(odd, high, low)


def x_halo(a_in, b_in, z, index, size, row):
    odd = index % 2 == 1
    zero = jnp.zeros((SUB, LANES), jnp.float32)
    before = jnp.where(index > 0, jnp.where(odd, a_in[z], b_in[z]), zero)
    after = jnp.where(index < size - 1, jnp.where(odd, b_in[z], a_in[z]), zero)
    up = SUB - 1 - row

    def merge(depth, shift):
        lo = pltpu.roll(before, shift, 0) if shift else before
        hi = pltpu.roll(after, SUB - shift, 0) if shift else after
        return jnp.where(row < depth, hi, jnp.where(up < depth, lo, 0.0))

    return merge(DEPTH, 0), merge(DEPTH, DEPTH), merge(DEPTH - 1, 2 * DEPTH)


def packed_place(lane, lz):
    group = lane // GROUP
    inside = group < -(-(lz + DEPTH) // STRIDE)
    return jnp.where(inside, group, -1), jnp.where(inside, lane - GROUP * group, -1)


def pack_own(tiles, group, place, sweep):
    zero = jnp.zeros((SUB, LANES), jnp.float32)
    raw = jnp.where(place < 2 * OWN, group, -1)
    levels = tiles[0]
    count = tiles[1]
    acc = [[[zero] * count for _ in range(STRIDE)] for _ in range(3)]
    for z in range(levels):
        g, v = z // STRIDE, z % STRIDE
        for f in range(3):
            for t, tile in enumerate(sweep(f, z)):
                if tile is not None:
                    acc[f][v][t] = jnp.where(
                        raw == g, pltpu.roll(tile, (GROUP * g + OWN) % LANES, 1), acc[f][v][t]
                    )
    own = [[[None] * count for _ in range(STRIDE)] for _ in range(3)]
    sides = [[[None] * count for _ in range(STRIDE)] for _ in range(2)]
    for v in range(STRIDE):
        base = GROUP // 2 if v == 1 else 0
        at = place - base
        for t in range(count):
            for f in range(3):
                a = acc[f][v][t]
                moved = pltpu.roll(a, GROUP - 2 * OWN, 1)
                own[f][v][t] = jnp.where(
                    place < OWN, a, jnp.where(place >= GROUP - OWN, moved, 0.0)
                )
            for side, first in enumerate((DEPTH, OWN)):
                b, h, c = (
                    pltpu.roll(acc[f][v][t], (LANES + base + k * DEPTH - first) % LANES, 1)
                    if (base + k * DEPTH - first) % LANES
                    else acc[f][v][t]
                    for k, f in enumerate((1, 2, 0))
                )
                sides[side][v][t] = jnp.where(at < DEPTH, b, jnp.where(at < 2 * DEPTH, h, c))
    return own, sides


def put_messages(ya, yb, sides, place, odd, t, row):
    rows = tile_rows(row)
    for i, pick in enumerate((lambda s: jnp.where(place < GROUP // 2, s[0][t], s[1][t]),
                              lambda s: s[2][t])):
        upper, lower = pick(sides[0]), pick(sides[1])
        ya[i, rows, :] = jnp.where(odd, lower, upper)
        yb[i, rows, :] = jnp.where(odd, upper, lower)


def pack_block_kernel(c_in, b_in, h_in, zin, pc_out, pb_out, ph_out, ya, yb):
    lz, lx, _ = c_in.shape
    group, place = packed_place(iota(1), lz)
    odd = lax.axis_index("gy") % 2 == 1
    tiles = lx // SUB

    def sweep(f, z):
        ref, i = local_or_z(*(
            (c_in, zin, 2 * DEPTH, DEPTH - 1, z),
            (b_in, zin, 0, DEPTH, z),
            (h_in, zin, DEPTH, DEPTH, z),
        )[f])
        return [None if ref is None else ref[i, tile_rows(t), :] for t in range(tiles)]

    own, sides = pack_own((lz + DEPTH, tiles), group, place, sweep)
    for t in range(tiles):
        for f, ref in enumerate((pc_out, pb_out, ph_out)):
            for v in range(STRIDE):
                ref[v, tile_rows(t), :] = own[f][v][t]
        put_messages(ya, yb, sides, place, odd, t, t)


def pack_halo_kernel(nx, lz, xa, xb, ya_in, yb_in, pc_out, pb_out, ph_out, ya, yb):
    ix = lax.axis_index("gx")
    group, place = packed_place(iota(1), lz)
    odd = lax.axis_index("gy") % 2 == 1
    row = iota(0)
    parts = {}

    def sweep(f, z):
        if z not in parts:
            parts[z] = x_halo(xa, xb, z, ix, nx, row)
        return [parts[z][(f + 2) % 3]]

    own, sides = pack_own((lz + DEPTH, 1), group, place, sweep)
    for f, ref in enumerate((pc_out, pb_out, ph_out)):
        for v in range(STRIDE):
            ref[v] = own[f][v][0]
    put_messages(ya, yb, sides, place, odd, 0, 0)
    for src, dst in ((ya_in, ya), (yb_in, yb)):
        for i in range(STRIDE - 1):
            for t in range(src.shape[1] // SUB):
                dst[i, tile_rows(t + 1), :] = src[i, tile_rows(t), :]


def main_kernel(nx, c_in, b_in, h_in, zin, xa, xb, it_out, s_out, cm, bm, hm, y1, y2, h1, h2):
    lz, lx, _ = it_out.shape
    tiles = lx // SUB + 1
    halo = tile_rows(tiles)
    zero = jnp.zeros((SUB, LANES), jnp.float32)
    ix, row = lax.axis_index("gx"), iota(0)
    for z in range(lz + DEPTH):
        parts = x_halo(xa, xb, z, ix, nx, row)
        local = (
            local_or_z(b_in, zin, 0, DEPTH, z),
            local_or_z(h_in, zin, DEPTH, DEPTH, z),
            local_or_z(c_in, zin, 2 * DEPTH, DEPTH - 1, z),
        )
        for f, store in enumerate((bm, hm, cm)):
            ref, i = local[f]
            for t in range(tiles):
                if t == 0:
                    tile = parts[f]
                    store[z, halo, :] = tile
                else:
                    tile = zero if ref is None else ref[i, tile_rows(t - 1), :]
                store[z, tile_rows(t), :] = tile
    for store in (cm, bm, hm):
        for t in range(tiles + 1):
            store[lz + DEPTH, tile_rows(t), :] = zero

    def spread(v, z, t):
        rows = tile_rows(t)
        here = v[z, rows, :]
        at = SUB * (tiles if t == 0 else t) - 1
        total = v[z, at : at + SUB, :] + v[z, SUB * t + 1 : SUB * t + 1 + SUB, :]
        total = total + (v[z - 1, rows, :] + v[z + 1, rows, :])
        sides = pltpu.roll(here, 1, 1) + pltpu.roll(here, LANES - 1, 1)
        return total + sides, here

    def step(v, source, out, start):
        for z in range(start, lz + DEPTH):
            for t in range(tiles):
                rows = tile_rows(t)
                total, here = spread(v, z, t)
                value = cm[z, rows, :] * total
                if source is not None:
                    value = source[z, rows, :] + value
                value = KEEP * here + value
                out[z, rows, :] = value
                if t == 0:
                    out[z, halo, :] = value
        for t in range(tiles + 1):
            out[lz + DEPTH, tile_rows(t), :] = zero

    step(hm, None, h1, 1)
    step(bm, bm, y1, 1)
    step(h1, None, h2, 2)
    step(y1, bm, y2, 2)
    for z in range(DEPTH, lz + DEPTH):
        for t in range(1, tiles):
            rows, block = tile_rows(t), tile_rows(t - 1)
            k = z - DEPTH
            c, b = cm[z, rows, :], bm[z, rows, :]
            total_h, g2 = spread(h2, z, t)
            total_y, x3 = spread(y2, z, t)
            x2 = y1[z, rows, :]
            g1 = KEEP * g2 + c * total_h
            w3 = b + c * total_y
            it_out[k, block, :] = KEEP * x3 + w3
            s_out[k, block, :] = (g1 * b + g2 * (x2 - KEEP * b)) + (
                h1[z, rows, :] * (x3 - KEEP * x2) + hm[z, rows, :] * w3
            )


def edge_kernel(ny, pc, pb, ph, qc, qb, qh, ya, yb, it_in, s_in, e_in, land_in, it_hbm, rg_hbm,
                cs, bs, hs, y1, y2, h1, h2, it_out, rg_out, sem):
    lz, lx, _ = e_in.shape
    iy = lax.axis_index("gy")
    lane = iota(1)
    group, place = packed_place(lane, lz)
    tiles = lx // SUB + 1
    halo = tile_rows(tiles)
    zero = jnp.zeros((SUB, LANES), jnp.float32)
    odd = iy % 2 == 1
    after = (place >= OWN) & (place < OWN + DEPTH)
    before = (place >= OWN + DEPTH) & (place < OWN + 2 * DEPTH)

    def put(ref, v, t, value):
        ref[v, tile_rows(t), :] = value
        if t == 0:
            ref[v, halo, :] = value

    for v in range(STRIDE):
        for t in range(tiles):
            rows = tile_rows(t)
            a, b = ya[v // 2, rows, :], yb[v // 2, rows, :]
            lo = jnp.where(iy > 0, jnp.where(odd, a, b), zero)
            hi = jnp.where(iy < ny - 1, jnp.where(odd, b, a), zero)
            base = GROUP // 2 if v == 1 else 0
            for k, (ref, block, tile) in enumerate(((bs, pb, qb), (hs, ph, qh), (cs, pc, qc))):
                own = tile[v] if t == 0 else block[v, tile_rows(t - 1), :]
                shift = OWN - k * DEPTH - base
                from_lo = pltpu.roll(lo, (shift + DEPTH) % LANES, 1)
                from_hi = pltpu.roll(hi, shift % LANES, 1) if shift else hi
                put(ref, v, t, jnp.where(before, from_lo, jnp.where(after, from_hi, own)))

    def spread(ref, v, t):
        rows = tile_rows(t)
        here = ref[v, rows, :]
        at = SUB * (tiles if t == 0 else t) - 1
        total = ref[v, at : at + SUB, :] + ref[v, SUB * t + 1 : SUB * t + 1 + SUB, :]
        down = ref[(v - 1) % STRIDE, rows, :]
        up = ref[(v + 1) % STRIDE, rows, :]
        if v == 0:
            down = pltpu.roll(down, GROUP, 1)
        if v == STRIDE - 1:
            up = pltpu.roll(up, LANES - GROUP, 1)
        sides = pltpu.roll(here, 1, 1) + pltpu.roll(here, LANES - 1, 1)
        return total + (down + up) + sides, here

    def step(src, source, out):
        for v in range(STRIDE):
            for t in range(tiles):
                rows = tile_rows(t)
                total, here = spread(src, v, t)
                value = cs[v, rows, :] * total
                if source is not None:
                    value = source[v, rows, :] + value
                put(out, v, t, KEEP * here + value)

    step(hs, None, h1)
    step(bs, bs, y1)
    step(h1, None, h2)
    step(y1, bs, y2)
    its, ss = {}, {}
    for v in range(STRIDE):
        for t in range(1, tiles):
            rows = tile_rows(t)
            c, b = cs[v, rows, :], bs[v, rows, :]
            total_h, g2 = spread(h2, v, t)
            total_y, x3 = spread(y2, v, t)
            x2 = y1[v, rows, :]
            g1 = KEEP * g2 + c * total_h
            w3 = b + c * total_y
            it = KEEP * x3 + w3
            s = (g1 * b + g2 * (x2 - KEEP * b)) + (
                h1[v, rows, :] * (x3 - KEEP * x2) + hs[v, rows, :] * w3
            )
            its[v, t] = jnp.where(place < OWN, it, pltpu.roll(it, LANES - OWN, 1))
            ss[v, t] = jnp.where(place < OWN, s, pltpu.roll(s, LANES - OWN, 1))
    rim = (lane < DEPTH) | (lane >= LANES - DEPTH)
    copies = []
    for k in range(lz):
        z = level(k, lz)
        g, v = (k + DEPTH) // STRIDE, (k + DEPTH) % STRIDE
        shift = (LANES - DEPTH - (GROUP * g + DEPTH)) % LANES
        for t in range(1, tiles):
            block = tile_rows(t - 1)
            it = jnp.where(rim, pltpu.roll(its[v, t], shift, 1), it_in[k, block, :])
            s = jnp.where(rim, pltpu.roll(ss[v, t], shift, 1), s_in[k, block, :])
            it_out[k, block, :] = it + land_in[k, block, :]
            rg_out[k, block, :] = e_in[k, block, :] * s
        for i, (a, b) in enumerate(((it_out, it_hbm), (rg_out, rg_hbm))):
            copies.append(pltpu.make_async_copy(a.at[k], b.at[z], sem.at[i, k]))
            copies[-1].start()
    for copy in copies:
        copy.wait()


def body(nx, ny, log_range, sea_mask, forcing, cotangent):
    lz, lx, ly = forcing.shape
    f32 = jnp.float32
    sizes = (nx, ny, 2)
    vmem = pl.BlockSpec(memory_space=pltpu.VMEM)
    hbm = pl.BlockSpec(memory_space=pltpu.HBM)

    def call(kernel, shapes, args, name, scratch=(), flops=10**6, ins=vmem, outs=vmem):
        return pl.pallas_call(
            kernel,
            out_shape=[jax.ShapeDtypeStruct(s, f32) for s in shapes],
            in_specs=[ins] * len(args),
            out_specs=[outs] * len(shapes),
            scratch_shapes=[pltpu.VMEM(s, f32) if isinstance(s, tuple) else s for s in scratch],
            compiler_params=pltpu.CompilerParams(vmem_limit_bytes=16 * 2**20),
            cost_estimate=pl.CostEstimate(flops=flops, bytes_accessed=2**20, transcendentals=0),
            name=name,
        )(*args)

    block = (lz, lx, ly)
    store = (lz + DEPTH + 1, lx + 2 * SUB, ly)
    strip = (STRIDE, lx + 2 * SUB, LANES)
    c, b, h, e, land, zmsg = call(
        prepare_kernel,
        [block] * 5 + [(3 * DEPTH - 1, lx, ly)],
        [
            pltpu.with_memory_space_constraint(a, pltpu.HBM)
            for a in (log_range, sea_mask, forcing, cotangent)
        ],
        "prepare",
        [block, pltpu.VMEM(block, jnp.int32), block, block, pltpu.SemaphoreType.DMA((4,))],
        ins=hbm,
    )
    swap = [(d, d ^ 1) for d in range(2 * nx * ny)]
    zin = lax.ppermute(zmsg, AXES, swap)
    xa, xb = call(pack_x_kernel, [(lz + DEPTH, SUB, ly)] * 2, (c, b, h, zin), "pack_x")
    xa = lax.ppermute(xa, AXES, pair_swaps(sizes, 0, 0))
    xb = lax.ppermute(xb, AXES, pair_swaps(sizes, 0, 1))
    pc, pb, ph, ya, yb = call(
        pack_block_kernel,
        [(STRIDE, lx, LANES)] * 3 + [(STRIDE - 1, lx, LANES)] * 2,
        (c, b, h, zin),
        "pack_block",
        flops=10**8,
    )
    qc, qb, qh, ya, yb = call(
        functools.partial(pack_halo_kernel, nx, lz),
        [(STRIDE, SUB, LANES)] * 3 + [(STRIDE - 1, lx + SUB, LANES)] * 2,
        (xa, xb, ya, yb),
        "pack_halo",
    )
    ya = lax.ppermute(ya, AXES, pair_swaps(sizes, 1, 0))
    yb = lax.ppermute(yb, AXES, pair_swaps(sizes, 1, 1))
    it, s = call(
        functools.partial(main_kernel, nx),
        [block] * 2,
        (c, b, h, zin, xa, xb),
        "main",
        [store] * 7,
        flops=2 * 10**8,
    )
    return call(
        functools.partial(edge_kernel, ny),
        [block] * 2,
        (pc, pb, ph, qc, qb, qh, ya, yb, it, s, e, land),
        "edge",
        [strip] * 7 + [block] * 2 + [pltpu.SemaphoreType.DMA((2, lz))],
        outs=hbm,
    )


def solution(mesh):
    nx, ny = mesh.shape["gx"], mesh.shape["gy"]
    spec = P("gz", "gx", "gy")
    return jax.shard_map(
        lambda *args: tuple(body(nx, ny, *args)),
        mesh=mesh,
        in_specs=(spec,) * 4,
        out_specs=(spec,) * 2,
        check_vma=False,
    )
```

```python
import functools

import jax
import jax.numpy as jnp
from jax import lax
from jax.experimental import pallas as pl
from jax.experimental.pallas import tpu as pltpu
from jax.sharding import PartitionSpec as P

SWEEPS = 4
RELAX = 0.9
KEEP = 1.0 - RELAX
SUB, LANES, DEPTH = 8, 128, SWEEPS - 1
OWN = 2 * DEPTH
GROUP = 2 * (OWN + DEPTH)
STRIDE = 3
AXES = ("gx", "gy", "gz")
ALL = slice(None)


def pair_swaps(sizes, axis, parity):
    nx, ny, nz = sizes
    pairs = []
    for i in range(nx):
        for j in range(ny):
            for k in range(nz):
                to = [i, j, k]
                other = to[axis] + (1 if to[axis] % 2 == parity else -1)
                if 0 <= other < sizes[axis]:
                    to[axis] = other
                else:
                    to[2] = 1 - k
                pairs.append(((i * ny + j) * nz + k, (to[0] * ny + to[1]) * nz + to[2]))
    return pairs


def iota(dim):
    return lax.broadcasted_iota(jnp.int32, (SUB, LANES), dim)


def level(t, lz):
    return jnp.where(lax.axis_index("gz") == 0, lz - 1 - t, t)


def tile_rows(t):
    return slice(SUB * t, SUB * (t + 1))


def coefficients(log_range, sea, source, cotangent):
    wet = sea != 0
    decay = jnp.exp(-2.0 * log_range)
    c = jnp.where(wet, RELAX / (6.0 + decay), 0.0)
    return wet, decay, c, c * source, c * cotangent


def prepare_z_kernel(lr_h, sea_h, src_h, cot_h, z_out, lr, sea, src, cot, sem):
    lz, lx = lr_h.shape[0], lr_h.shape[1]
    low = lax.axis_index("gz") == 0
    start = jnp.where(low, lz - DEPTH, 0)
    copies = [
        pltpu.make_async_copy(a.at[pl.ds(start, DEPTH)], b, sem.at[i])
        for i, (a, b) in enumerate(((lr_h, lr), (sea_h, sea), (src_h, src), (cot_h, cot)))
    ]
    for copy in copies:
        copy.start()
    for copy in copies:
        copy.wait()
    for t in range(DEPTH):
        z = jnp.where(low, DEPTH - 1 - t, t)
        for r in range(lx // SUB):
            rows = tile_rows(r)
            _, _, c, b, h = coefficients(
                lr[z, rows, :], sea[z, rows, :], src[z, rows, :], cot[z, rows, :]
            )
            z_out[t, rows, :] = b
            z_out[DEPTH + t, rows, :] = h
            if t < DEPTH - 1:
                z_out[2 * DEPTH + t, rows, :] = c


def prepare_kernel(lr, sea, src, cot, c_out, b_out, h_out, e_out, land_out):
    lz, lx, _ = lr.shape
    for t in range(lz):
        z = level(t, lz)
        for r in range(lx // SUB):
            rows = tile_rows(r)
            f = src[z, rows, :]
            wet, decay, c, b, h = coefficients(
                lr[z, rows, :], sea[z, rows, :], f, cot[z, rows, :]
            )
            c_out[t, rows, :] = c
            b_out[t, rows, :] = b
            h_out[t, rows, :] = h
            e_out[t, rows, :] = jnp.where(wet, (2.0 / RELAX) * decay, 0.0)
            land_out[t, rows, :] = jnp.where(
                wet, 0.0, RELAX * (1.0 + KEEP + KEEP**2 + KEEP**3) * f
            )


def local_or_z(local, zin, base, depth, z):
    if z >= DEPTH:
        return local, z - DEPTH
    t = DEPTH - 1 - z
    return (zin, base + t) if t < depth else (None, 0)


FACE = ((DEPTH, 0), (DEPTH, DEPTH), (DEPTH - 1, 2 * DEPTH))
CORNER = {1: ((2, 0), (2, 3), (1, 6)), 2: ((1, 2), (1, 5), (0, 0))}


def pack_x_kernel(c_in, b_in, h_in, zin, a_out, b_out):
    lz, lx, _ = c_in.shape
    odd = lax.axis_index("gx") % 2 == 1
    row = iota(0)
    for z in range(lz + 1):
        faces = []
        for rows, s in ((slice(0, SUB), 1), (slice(lx - SUB, lx), -1)):
            at = row if s == 1 else SUB - 1 - row
            if z < lz:
                parts = [(r[z, rows, :], q) for r, (_, q) in zip((b_in, h_in, c_in), FACE)]
            else:
                parts = [
                    (zin[DEPTH * f + t - 1, rows, :], CORNER[t][f][1])
                    for f in range(3)
                    for t in CORNER
                    if CORNER[t][f][0]
                ]
            parts.sort(key=lambda part: -part[1])
            face = None
            for tile, place in parts:
                if place:
                    tile = pltpu.roll(tile, (s * place) % SUB, 0)
                face = tile if face is None else jnp.where(at < limit, tile, face)
                limit = place
            faces.append(face)
        low, high = faces
        a_out[z] = jnp.where(odd, low, high)
        b_out[z] = jnp.where(odd, high, low)


def x_halo(a_in, b_in, z, index, size, row):
    zero = jnp.zeros((SUB, LANES), jnp.float32)
    if z >= DEPTH:
        at, fields = z - DEPTH, FACE
    else:
        at, fields = a_in.shape[0] - 1, CORNER.get(DEPTH - z)
    if fields is None:
        return zero, zero, zero
    odd = index % 2 == 1
    before = jnp.where(index > 0, jnp.where(odd, a_in[at], b_in[at]), zero)
    after = jnp.where(index < size - 1, jnp.where(odd, b_in[at], a_in[at]), zero)
    up = SUB - 1 - row

    def merge(depth, shift):
        if not depth:
            return zero
        lo = pltpu.roll(before, shift, 0) if shift else before
        hi = pltpu.roll(after, SUB - shift, 0) if shift else after
        return jnp.where(row < depth, hi, jnp.where(up < depth, lo, 0.0))

    return tuple(merge(*field) for field in fields)


def packed_place(lane, lz):
    group = lane // GROUP
    inside = group < -(-(lz + DEPTH) // STRIDE)
    return jnp.where(inside, group, -1), jnp.where(inside, lane - GROUP * group, -1)


def pack_own(tiles, group, place, sweep):
    zero = jnp.zeros((SUB, LANES), jnp.float32)
    raw = jnp.where(place < 2 * OWN, group, -1)
    levels = tiles[0]
    count = tiles[1]
    acc = [[[zero] * count for _ in range(STRIDE)] for _ in range(3)]
    for z in range(levels):
        g, v = z // STRIDE, z % STRIDE
        for f in range(3):
            for t, tile in enumerate(sweep(f, z)):
                if tile is not None:
                    acc[f][v][t] = jnp.where(
                        raw == g, pltpu.roll(tile, (GROUP * g + OWN) % LANES, 1), acc[f][v][t]
                    )
    own = [[[None] * count for _ in range(STRIDE)] for _ in range(3)]
    sides = [[[None] * count for _ in range(STRIDE)] for _ in range(2)]
    for v in range(STRIDE):
        base = GROUP // 2 if v == 1 else 0
        at = place - base
        for t in range(count):
            for f in range(3):
                a = acc[f][v][t]
                moved = pltpu.roll(a, GROUP - 2 * OWN, 1)
                own[f][v][t] = jnp.where(
                    place < OWN, a, jnp.where(place >= GROUP - OWN, moved, 0.0)
                )
            for side, first in enumerate((DEPTH, OWN)):
                b, h, c = (
                    pltpu.roll(acc[f][v][t], (LANES + base + k * DEPTH - first) % LANES, 1)
                    if (base + k * DEPTH - first) % LANES
                    else acc[f][v][t]
                    for k, f in enumerate((1, 2, 0))
                )
                sides[side][v][t] = jnp.where(at < DEPTH, b, jnp.where(at < 2 * DEPTH, h, c))
    return own, sides


def put_messages(ya, yb, sides, place, odd, t, row):
    rows = tile_rows(row)
    for i, pick in enumerate((lambda s: jnp.where(place < GROUP // 2, s[0][t], s[1][t]),
                              lambda s: s[2][t])):
        upper, lower = pick(sides[0]), pick(sides[1])
        ya[i, rows, :] = jnp.where(odd, lower, upper)
        yb[i, rows, :] = jnp.where(odd, upper, lower)


def pack_block_kernel(c_in, b_in, h_in, zin, pc_out, pb_out, ph_out, ya, yb):
    lz, lx, _ = c_in.shape
    group, place = packed_place(iota(1), lz)
    odd = lax.axis_index("gy") % 2 == 1
    tiles = lx // SUB

    def sweep(f, z):
        ref, i = local_or_z(*(
            (c_in, zin, 2 * DEPTH, DEPTH - 1, z),
            (b_in, zin, 0, DEPTH, z),
            (h_in, zin, DEPTH, DEPTH, z),
        )[f])
        return [None if ref is None else ref[i, tile_rows(t), :] for t in range(tiles)]

    own, sides = pack_own((lz + DEPTH, tiles), group, place, sweep)
    for t in range(tiles):
        for f, ref in enumerate((pc_out, pb_out, ph_out)):
            for v in range(STRIDE):
                ref[v, tile_rows(t), :] = own[f][v][t]
        put_messages(ya, yb, sides, place, odd, t, t)


def pack_halo_kernel(nx, lz, xa, xb, ya_in, yb_in, pc_out, pb_out, ph_out, ya, yb):
    ix = lax.axis_index("gx")
    group, place = packed_place(iota(1), lz)
    odd = lax.axis_index("gy") % 2 == 1
    row = iota(0)
    parts = {}

    def sweep(f, z):
        if z not in parts:
            parts[z] = x_halo(xa, xb, z, ix, nx, row)
        return [parts[z][(f + 2) % 3]]

    own, sides = pack_own((lz + DEPTH, 1), group, place, sweep)
    for f, ref in enumerate((pc_out, pb_out, ph_out)):
        for v in range(STRIDE):
            ref[v] = own[f][v][0]
    put_messages(ya, yb, sides, place, odd, 0, 0)
    for src, dst in ((ya_in, ya), (yb_in, yb)):
        for i in range(STRIDE - 1):
            for t in range(src.shape[1] // SUB):
                dst[i, tile_rows(t + 1), :] = src[i, tile_rows(t), :]


def main_kernel(nx, c_in, b_in, h_in, zin, xa, xb, it_out, s_out, cm, bm, hm, y1, y2, h1, h2):
    lz, lx, _ = it_out.shape
    tiles = lx // SUB + 1
    halo = tile_rows(tiles)
    zero = jnp.zeros((SUB, LANES), jnp.float32)
    ix, row = lax.axis_index("gx"), iota(0)
    for z in range(lz + DEPTH):
        parts = x_halo(xa, xb, z, ix, nx, row)
        local = (
            local_or_z(b_in, zin, 0, DEPTH, z),
            local_or_z(h_in, zin, DEPTH, DEPTH, z),
            local_or_z(c_in, zin, 2 * DEPTH, DEPTH - 1, z),
        )
        for f, store in enumerate((bm, hm, cm)):
            ref, i = local[f]
            for t in range(tiles):
                if t == 0:
                    tile = parts[f]
                    store[z, halo, :] = tile
                else:
                    tile = zero if ref is None else ref[i, tile_rows(t - 1), :]
                store[z, tile_rows(t), :] = tile
    for store in (cm, bm, hm):
        for t in range(tiles + 1):
            store[lz + DEPTH, tile_rows(t), :] = zero

    def spread(v, z, t):
        rows = tile_rows(t)
        here = v[z, rows, :]
        at = SUB * (tiles if t == 0 else t) - 1
        total = v[z, at : at + SUB, :] + v[z, SUB * t + 1 : SUB * t + 1 + SUB, :]
        total = total + (v[z - 1, rows, :] + v[z + 1, rows, :])
        sides = pltpu.roll(here, 1, 1) + pltpu.roll(here, LANES - 1, 1)
        return total + sides, here

    def step(v, source, out, start):
        for z in range(start, lz + DEPTH):
            for t in range(tiles):
                rows = tile_rows(t)
                total, here = spread(v, z, t)
                value = cm[z, rows, :] * total
                if source is not None:
                    value = source[z, rows, :] + value
                value = KEEP * here + value
                out[z, rows, :] = value
                if t == 0:
                    out[z, halo, :] = value
        for t in range(tiles + 1):
            out[lz + DEPTH, tile_rows(t), :] = zero

    step(hm, None, h1, 1)
    step(bm, bm, y1, 1)
    step(h1, None, h2, 2)
    step(y1, bm, y2, 2)
    for z in range(DEPTH, lz + DEPTH):
        for t in range(1, tiles):
            rows, block = tile_rows(t), tile_rows(t - 1)
            k = z - DEPTH
            c, b = cm[z, rows, :], bm[z, rows, :]
            total_h, g2 = spread(h2, z, t)
            total_y, x3 = spread(y2, z, t)
            x2 = y1[z, rows, :]
            g1 = KEEP * g2 + c * total_h
            w3 = b + c * total_y
            it_out[k, block, :] = KEEP * x3 + w3
            s_out[k, block, :] = (g1 * b + g2 * (x2 - KEEP * b)) + (
                h1[z, rows, :] * (x3 - KEEP * x2) + hm[z, rows, :] * w3
            )


def edge_kernel(ny, pc, pb, ph, qc, qb, qh, ya, yb, it_in, s_in, e_in, land_in, it_hbm, rg_hbm,
                cs, bs, hs, y1, y2, h1, h2, it_out, rg_out, sem):
    lz, lx, _ = e_in.shape
    iy = lax.axis_index("gy")
    lane = iota(1)
    group, place = packed_place(lane, lz)
    tiles = lx // SUB + 1
    halo = tile_rows(tiles)
    zero = jnp.zeros((SUB, LANES), jnp.float32)
    odd = iy % 2 == 1
    after = (place >= OWN) & (place < OWN + DEPTH)
    before = (place >= OWN + DEPTH) & (place < OWN + 2 * DEPTH)

    def put(ref, v, t, value):
        ref[v, tile_rows(t), :] = value
        if t == 0:
            ref[v, halo, :] = value

    for v in range(STRIDE):
        for t in range(tiles):
            rows = tile_rows(t)
            a, b = ya[v // 2, rows, :], yb[v // 2, rows, :]
            lo = jnp.where(iy > 0, jnp.where(odd, a, b), zero)
            hi = jnp.where(iy < ny - 1, jnp.where(odd, b, a), zero)
            base = GROUP // 2 if v == 1 else 0
            for k, (ref, block, tile) in enumerate(((bs, pb, qb), (hs, ph, qh), (cs, pc, qc))):
                own = tile[v] if t == 0 else block[v, tile_rows(t - 1), :]
                shift = OWN - k * DEPTH - base
                from_lo = pltpu.roll(lo, (shift + DEPTH) % LANES, 1)
                from_hi = pltpu.roll(hi, shift % LANES, 1) if shift else hi
                put(ref, v, t, jnp.where(before, from_lo, jnp.where(after, from_hi, own)))

    def spread(ref, v, t):
        rows = tile_rows(t)
        here = ref[v, rows, :]
        at = SUB * (tiles if t == 0 else t) - 1
        total = ref[v, at : at + SUB, :] + ref[v, SUB * t + 1 : SUB * t + 1 + SUB, :]
        down = ref[(v - 1) % STRIDE, rows, :]
        up = ref[(v + 1) % STRIDE, rows, :]
        if v == 0:
            down = pltpu.roll(down, GROUP, 1)
        if v == STRIDE - 1:
            up = pltpu.roll(up, LANES - GROUP, 1)
        sides = pltpu.roll(here, 1, 1) + pltpu.roll(here, LANES - 1, 1)
        return total + (down + up) + sides, here

    def step(src, source, out):
        for v in range(STRIDE):
            for t in range(tiles):
                rows = tile_rows(t)
                total, here = spread(src, v, t)
                value = cs[v, rows, :] * total
                if source is not None:
                    value = source[v, rows, :] + value
                put(out, v, t, KEEP * here + value)

    step(hs, None, h1)
    step(bs, bs, y1)
    step(h1, None, h2)
    step(y1, bs, y2)
    its, ss = {}, {}
    for v in range(STRIDE):
        for t in range(1, tiles):
            rows = tile_rows(t)
            c, b = cs[v, rows, :], bs[v, rows, :]
            total_h, g2 = spread(h2, v, t)
            total_y, x3 = spread(y2, v, t)
            x2 = y1[v, rows, :]
            g1 = KEEP * g2 + c * total_h
            w3 = b + c * total_y
            it = KEEP * x3 + w3
            s = (g1 * b + g2 * (x2 - KEEP * b)) + (
                h1[v, rows, :] * (x3 - KEEP * x2) + hs[v, rows, :] * w3
            )
            its[v, t] = jnp.where(place < OWN, it, pltpu.roll(it, LANES - OWN, 1))
            ss[v, t] = jnp.where(place < OWN, s, pltpu.roll(s, LANES - OWN, 1))
    rim = (lane < DEPTH) | (lane >= LANES - DEPTH)
    copies = []
    for k in range(lz):
        z = level(k, lz)
        g, v = (k + DEPTH) // STRIDE, (k + DEPTH) % STRIDE
        shift = (LANES - DEPTH - (GROUP * g + DEPTH)) % LANES
        for t in range(1, tiles):
            block = tile_rows(t - 1)
            it = jnp.where(rim, pltpu.roll(its[v, t], shift, 1), it_in[k, block, :])
            s = jnp.where(rim, pltpu.roll(ss[v, t], shift, 1), s_in[k, block, :])
            it_out[k, block, :] = it + land_in[k, block, :]
            rg_out[k, block, :] = e_in[k, block, :] * s
        for i, (a, b) in enumerate(((it_out, it_hbm), (rg_out, rg_hbm))):
            copies.append(pltpu.make_async_copy(a.at[k], b.at[z], sem.at[i, k]))
            copies[-1].start()
    for copy in copies:
        copy.wait()


def body(nx, ny, log_range, sea_mask, forcing, cotangent):
    lz, lx, ly = forcing.shape
    f32 = jnp.float32
    sizes = (nx, ny, 2)
    vmem = pl.BlockSpec(memory_space=pltpu.VMEM)
    hbm = pl.BlockSpec(memory_space=pltpu.HBM)

    def call(kernel, shapes, args, name, scratch=(), flops=10**6, ins=vmem, outs=vmem):
        return pl.pallas_call(
            kernel,
            out_shape=[jax.ShapeDtypeStruct(s, f32) for s in shapes],
            in_specs=[ins] * len(args),
            out_specs=[outs] * len(shapes),
            scratch_shapes=[pltpu.VMEM(s, f32) if isinstance(s, tuple) else s for s in scratch],
            compiler_params=pltpu.CompilerParams(vmem_limit_bytes=16 * 2**20),
            cost_estimate=pl.CostEstimate(flops=flops, bytes_accessed=2**20, transcendentals=0),
            name=name,
        )(*args)

    block = (lz, lx, ly)
    store = (lz + DEPTH + 1, lx + 2 * SUB, ly)
    strip = (STRIDE, lx + 2 * SUB, LANES)
    args = (log_range, sea_mask, forcing, cotangent)
    face = (DEPTH, lx, ly)
    (zmsg,) = call(
        prepare_z_kernel,
        [(3 * DEPTH - 1, lx, ly)],
        [pltpu.with_memory_space_constraint(a, pltpu.HBM) for a in args],
        "prepare_z",
        [face, pltpu.VMEM(face, jnp.int32), face, face, pltpu.SemaphoreType.DMA((4,))],
        ins=hbm,
    )
    c, b, h, e, land = call(prepare_kernel, [block] * 5, args, "prepare", flops=10**8)
    swap = [(d, d ^ 1) for d in range(2 * nx * ny)]
    zin = lax.ppermute(zmsg, AXES, swap)
    xa, xb = call(pack_x_kernel, [(lz + 1, SUB, ly)] * 2, (c, b, h, zin), "pack_x")
    xa = lax.ppermute(xa, AXES, pair_swaps(sizes, 0, 0))
    xb = lax.ppermute(xb, AXES, pair_swaps(sizes, 0, 1))
    pc, pb, ph, ya, yb = call(
        pack_block_kernel,
        [(STRIDE, lx, LANES)] * 3 + [(STRIDE - 1, lx, LANES)] * 2,
        (c, b, h, zin),
        "pack_block",
        flops=10**8,
    )
    qc, qb, qh, ya, yb = call(
        functools.partial(pack_halo_kernel, nx, lz),
        [(STRIDE, SUB, LANES)] * 3 + [(STRIDE - 1, lx + SUB, LANES)] * 2,
        (xa, xb, ya, yb),
        "pack_halo",
    )
    ya = lax.ppermute(ya, AXES, pair_swaps(sizes, 1, 0))
    yb = lax.ppermute(yb, AXES, pair_swaps(sizes, 1, 1))
    it, s = call(
        functools.partial(main_kernel, nx),
        [block] * 2,
        (c, b, h, zin, xa, xb),
        "main",
        [store] * 7,
        flops=2 * 10**8,
    )
    return call(
        functools.partial(edge_kernel, ny),
        [block] * 2,
        (pc, pb, ph, qc, qb, qh, ya, yb, it, s, e, land),
        "edge",
        [strip] * 7 + [block] * 2 + [pltpu.SemaphoreType.DMA((2, lz))],
        outs=hbm,
    )


def solution(mesh):
    nx, ny = mesh.shape["gx"], mesh.shape["gy"]
    spec = P("gz", "gx", "gy")
    return jax.shard_map(
        lambda *args: tuple(body(nx, ny, *args)),
        mesh=mesh,
        in_specs=(spec,) * 4,
        out_specs=(spec,) * 2,
        check_vma=False,
    )
```

```python
import functools

import jax
import jax.numpy as jnp
from jax import lax
from jax.experimental import pallas as pl
from jax.experimental.pallas import tpu as pltpu
from jax.sharding import PartitionSpec as P

SWEEPS = 4
RELAX = 0.9
KEEP = 1.0 - RELAX
SUB, LANES, DEPTH = 8, 128, SWEEPS - 1
OWN = 2 * DEPTH
GROUP = 2 * (OWN + DEPTH)
STRIDE = 3
AXES = ("gx", "gy", "gz")
ALL = slice(None)


def pair_swaps(sizes, axis, parity):
    nx, ny, nz = sizes
    pairs = []
    for i in range(nx):
        for j in range(ny):
            for k in range(nz):
                to = [i, j, k]
                other = to[axis] + (1 if to[axis] % 2 == parity else -1)
                if 0 <= other < sizes[axis]:
                    to[axis] = other
                else:
                    to[2] = 1 - k
                pairs.append(((i * ny + j) * nz + k, (to[0] * ny + to[1]) * nz + to[2]))
    return pairs


def iota(dim):
    return lax.broadcasted_iota(jnp.int32, (SUB, LANES), dim)


def level(t, lz):
    return jnp.where(lax.axis_index("gz") == 0, lz - 1 - t, t)


def tile_rows(t):
    return slice(SUB * t, SUB * (t + 1))


def coefficients(log_range, sea, source, cotangent):
    wet = sea != 0
    decay = jnp.exp(-2.0 * log_range)
    c = jnp.where(wet, RELAX / (6.0 + decay), 0.0)
    return wet, decay, c, c * source, c * cotangent


def prepare_z_kernel(lr_h, sea_h, src_h, cot_h, z_out, lr, sea, src, cot, sem):
    lz, lx = lr_h.shape[0], lr_h.shape[1]
    low = lax.axis_index("gz") == 0
    start = jnp.where(low, lz - DEPTH, 0)
    copies = [
        pltpu.make_async_copy(a.at[pl.ds(start, DEPTH)], b, sem.at[i])
        for i, (a, b) in enumerate(((lr_h, lr), (sea_h, sea), (src_h, src), (cot_h, cot)))
    ]
    for copy in copies:
        copy.start()
    for copy in copies:
        copy.wait()
    for t in range(DEPTH):
        z = jnp.where(low, DEPTH - 1 - t, t)
        for r in range(lx // SUB):
            rows = tile_rows(r)
            _, _, c, b, h = coefficients(
                lr[z, rows, :], sea[z, rows, :], src[z, rows, :], cot[z, rows, :]
            )
            z_out[t, rows, :] = b
            z_out[DEPTH + t, rows, :] = h
            if t < DEPTH - 1:
                z_out[2 * DEPTH + t, rows, :] = c


def prepare_kernel(lr, sea, src, cot, c_out, b_out, h_out, e_out, land_out):
    lz, lx, _ = lr.shape
    for t in range(lz):
        z = level(t, lz)
        for r in range(lx // SUB):
            rows = tile_rows(r)
            f = src[z, rows, :]
            wet, decay, c, b, h = coefficients(
                lr[z, rows, :], sea[z, rows, :], f, cot[z, rows, :]
            )
            c_out[t, rows, :] = c
            b_out[t, rows, :] = b
            h_out[t, rows, :] = h
            e_out[t, rows, :] = jnp.where(wet, (2.0 / RELAX) * decay, 0.0)
            land_out[t, rows, :] = jnp.where(
                wet, 0.0, RELAX * (1.0 + KEEP + KEEP**2 + KEEP**3) * f
            )


def local_or_z(local, zin, base, depth, z):
    if z >= DEPTH:
        return local, z - DEPTH
    t = DEPTH - 1 - z
    return (zin, base + t) if t < depth else (None, 0)


FACE = ((DEPTH, 0), (DEPTH, DEPTH), (DEPTH - 1, 2 * DEPTH))
CORNER = {1: ((2, 0), (2, 3), (1, 6)), 2: ((1, 2), (1, 5), (0, 0))}


def pack_x_kernel(c_in, b_in, h_in, zin, a_out, b_out):
    lz, lx, _ = c_in.shape
    odd = lax.axis_index("gx") % 2 == 1
    row = iota(0)
    for z in range(lz + 1):
        faces = []
        for rows, s in ((slice(0, SUB), 1), (slice(lx - SUB, lx), -1)):
            at = row if s == 1 else SUB - 1 - row
            if z < lz:
                parts = [(r[z, rows, :], q) for r, (_, q) in zip((b_in, h_in, c_in), FACE)]
            else:
                parts = [
                    (zin[DEPTH * f + t - 1, rows, :], CORNER[t][f][1])
                    for f in range(3)
                    for t in CORNER
                    if CORNER[t][f][0]
                ]
            parts.sort(key=lambda part: -part[1])
            face = None
            for tile, place in parts:
                if place:
                    tile = pltpu.roll(tile, (s * place) % SUB, 0)
                face = tile if face is None else jnp.where(at < limit, tile, face)
                limit = place
            faces.append(face)
        low, high = faces
        a_out[z] = jnp.where(odd, low, high)
        b_out[z] = jnp.where(odd, high, low)


def x_halo(a_in, b_in, z, index, size, row):
    zero = jnp.zeros((SUB, LANES), jnp.float32)
    if z >= DEPTH:
        at, fields = z - DEPTH, FACE
    else:
        at, fields = a_in.shape[0] - 1, CORNER.get(DEPTH - z)
    if fields is None:
        return zero, zero, zero
    odd = index % 2 == 1
    before = jnp.where(index > 0, jnp.where(odd, a_in[at], b_in[at]), zero)
    after = jnp.where(index < size - 1, jnp.where(odd, b_in[at], a_in[at]), zero)
    up = SUB - 1 - row

    def merge(depth, shift):
        if not depth:
            return zero
        lo = pltpu.roll(before, shift, 0) if shift else before
        hi = pltpu.roll(after, SUB - shift, 0) if shift else after
        return jnp.where(row < depth, hi, jnp.where(up < depth, lo, 0.0))

    return tuple(merge(*field) for field in fields)


def packed_place(lane, lz):
    group = lane // GROUP
    inside = group < -(-(lz + DEPTH) // STRIDE)
    return jnp.where(inside, group, -1), jnp.where(inside, lane - GROUP * group, -1)


BLOCK_FIELDS = ((1, DEPTH, 0), (2, DEPTH, DEPTH), (0, DEPTH, 2 * DEPTH))
HALO_FIELDS = ((1, DEPTH - 1, 0), (2, DEPTH - 1, DEPTH - 1), (0, DEPTH - 2, 2 * DEPTH - 2))


def message_slot(v, t, tiles):
    if t == 0:
        return 0, OWN * v
    if v < STRIDE - 1:
        return t, GROUP // 2 * v
    return tiles + (t - 1) // 2, GROUP // 2 * ((t - 1) % 2)


def message_length(tiles):
    return tiles + tiles // 2


def lane_roll(x, shift):
    return pltpu.roll(x, shift % LANES, 1) if shift % LANES else x


def pack_own(levels, first, count, tiles, place, group, sweep):
    zero = jnp.zeros((SUB, LANES), jnp.float32)
    raw = jnp.where(place < 2 * OWN, group, -1)
    acc = [[[zero] * count for _ in range(STRIDE)] for _ in range(3)]
    for z in range(levels):
        g, v = z // STRIDE, z % STRIDE
        for f in range(3):
            for t, tile in enumerate(sweep(f, z)):
                if tile is not None:
                    acc[f][v][t] = jnp.where(
                        raw == g, pltpu.roll(tile, (GROUP * g + OWN) % LANES, 1), acc[f][v][t]
                    )
    own = [[[None] * count for _ in range(STRIDE)] for _ in range(3)]
    sides = [{}, {}]
    for t in range(count):
        fields = BLOCK_FIELDS if first + t else HALO_FIELDS
        for v in range(STRIDE):
            slot, base = message_slot(v, first + t, tiles)
            for side in range(2):
                message = sides[side].get(slot)
                for f, depth, offset in fields:
                    at = OWN - depth if side == 0 else OWN
                    part = lane_roll(acc[f][v][t], base + offset - at)
                    if message is None:
                        message = part
                    else:
                        message = jnp.where(place >= base + offset, part, message)
                sides[side][slot] = message
            for f in range(3):
                a = acc[f][v][t]
                moved = pltpu.roll(a, GROUP - 2 * OWN, 1)
                own[f][v][t] = jnp.where(
                    place < OWN, a, jnp.where(place >= GROUP - OWN, moved, 0.0)
                )
    return own, sides


def put_messages(ya, yb, sides, odd):
    for slot in sides[0]:
        upper, lower = sides[0][slot], sides[1][slot]
        ya[slot] = jnp.where(odd, lower, upper)
        yb[slot] = jnp.where(odd, upper, lower)


def pack_block_kernel(c_in, b_in, h_in, zin, pc_out, pb_out, ph_out, ya, yb):
    lz, lx, _ = c_in.shape
    group, place = packed_place(iota(1), lz)
    odd = lax.axis_index("gy") % 2 == 1
    tiles = lx // SUB

    def sweep(f, z):
        ref, i = local_or_z(*(
            (c_in, zin, 2 * DEPTH, DEPTH - 1, z),
            (b_in, zin, 0, DEPTH, z),
            (h_in, zin, DEPTH, DEPTH, z),
        )[f])
        return [None if ref is None else ref[i, tile_rows(t), :] for t in range(tiles)]

    own, sides = pack_own(lz + DEPTH, 1, tiles, tiles + 1, place, group, sweep)
    put_messages(ya, yb, sides, odd)
    for t in range(tiles):
        for f, ref in enumerate((pc_out, pb_out, ph_out)):
            for v in range(STRIDE):
                ref[v, tile_rows(t), :] = own[f][v][t]


def pack_halo_kernel(nx, lz, xa, xb, ya_in, yb_in, pc_out, pb_out, ph_out, yb, ya):
    ix = lax.axis_index("gx")
    group, place = packed_place(iota(1), lz)
    odd = lax.axis_index("gy") % 2 == 1
    row = iota(0)
    parts = {}

    def sweep(f, z):
        if z not in parts:
            parts[z] = x_halo(xa, xb, z, ix, nx, row)
        return [parts[z][(f + 2) % 3]]

    own, sides = pack_own(lz + DEPTH, 0, 1, 0, place, group, sweep)
    put_messages(ya, yb, sides, odd)
    for src, dst in ((ya_in, ya), (yb_in, yb)):
        for i in range(1, src.shape[0]):
            dst[i] = src[i]
    for f, ref in enumerate((pc_out, pb_out, ph_out)):
        for v in range(STRIDE):
            ref[v] = own[f][v][0]


def main_kernel(nx, c_in, b_in, h_in, zin, xa, xb, it_out, s_out, cm, bm, hm, y1, y2, h1, h2):
    lz, lx, _ = it_out.shape
    tiles = lx // SUB + 1
    halo = tile_rows(tiles)
    zero = jnp.zeros((SUB, LANES), jnp.float32)
    ix, row = lax.axis_index("gx"), iota(0)
    for z in range(lz + DEPTH):
        parts = x_halo(xa, xb, z, ix, nx, row)
        local = (
            local_or_z(b_in, zin, 0, DEPTH, z),
            local_or_z(h_in, zin, DEPTH, DEPTH, z),
            local_or_z(c_in, zin, 2 * DEPTH, DEPTH - 1, z),
        )
        for f, store in enumerate((bm, hm, cm)):
            ref, i = local[f]
            for t in range(tiles):
                if t == 0:
                    tile = parts[f]
                    store[z, halo, :] = tile
                else:
                    tile = zero if ref is None else ref[i, tile_rows(t - 1), :]
                store[z, tile_rows(t), :] = tile
    for store in (cm, bm, hm):
        for t in range(tiles + 1):
            store[lz + DEPTH, tile_rows(t), :] = zero

    def spread(v, z, t):
        rows = tile_rows(t)
        here = v[z, rows, :]
        at = SUB * (tiles if t == 0 else t) - 1
        total = v[z, at : at + SUB, :] + v[z, SUB * t + 1 : SUB * t + 1 + SUB, :]
        total = total + (v[z - 1, rows, :] + v[z + 1, rows, :])
        sides = pltpu.roll(here, 1, 1) + pltpu.roll(here, LANES - 1, 1)
        return total + sides, here

    def step(v, source, out, start):
        for z in range(start, lz + DEPTH):
            for t in range(tiles):
                rows = tile_rows(t)
                total, here = spread(v, z, t)
                value = cm[z, rows, :] * total
                if source is not None:
                    value = source[z, rows, :] + value
                value = KEEP * here + value
                out[z, rows, :] = value
                if t == 0:
                    out[z, halo, :] = value
        for t in range(tiles + 1):
            out[lz + DEPTH, tile_rows(t), :] = zero

    step(hm, None, h1, 1)
    step(bm, bm, y1, 1)
    step(h1, None, h2, 2)
    step(y1, bm, y2, 2)
    for z in range(DEPTH, lz + DEPTH):
        for t in range(1, tiles):
            rows, block = tile_rows(t), tile_rows(t - 1)
            k = z - DEPTH
            c, b = cm[z, rows, :], bm[z, rows, :]
            total_h, g2 = spread(h2, z, t)
            total_y, x3 = spread(y2, z, t)
            x2 = y1[z, rows, :]
            g1 = KEEP * g2 + c * total_h
            w3 = b + c * total_y
            it_out[k, block, :] = KEEP * x3 + w3
            s_out[k, block, :] = (g1 * b + g2 * (x2 - KEEP * b)) + (
                h1[z, rows, :] * (x3 - KEEP * x2) + hm[z, rows, :] * w3
            )


def edge_kernel(ny, pc, pb, ph, qc, qb, qh, yb, ya, it_in, s_in, e_in, land_in, it_hbm, rg_hbm,
                cs, bs, hs, y1, y2, h1, h2, it_out, rg_out, sem):
    lz, lx, _ = e_in.shape
    iy = lax.axis_index("gy")
    lane = iota(1)
    group, place = packed_place(lane, lz)
    tiles = lx // SUB + 1
    halo = tile_rows(tiles)
    zero = jnp.zeros((SUB, LANES), jnp.float32)
    odd = iy % 2 == 1

    def put(ref, v, t, value):
        ref[v, tile_rows(t), :] = value
        if t == 0:
            ref[v, halo, :] = value

    slots = []
    for i in range(ya.shape[0]):
        a, b = ya[i], yb[i]
        slots.append(
            (
                jnp.where(iy > 0, jnp.where(odd, a, b), zero),
                jnp.where(iy < ny - 1, jnp.where(odd, b, a), zero),
            )
        )
    stores = (cs, bs, hs)
    blocks, halos = (pc, pb, ph), (qc, qb, qh)
    for t in range(tiles):
        for v in range(STRIDE):
            slot, base = message_slot(v, t, tiles)
            lo, hi = slots[slot]
            for f, depth, offset in BLOCK_FIELDS if t else HALO_FIELDS:
                end = OWN + 2 * DEPTH
                before = (place >= end - depth) & (place < end)
                after = (place >= OWN) & (place < OWN + depth)
                from_lo = lane_roll(lo, end - depth - base - offset)
                from_hi = lane_roll(hi, OWN - base - offset)
                own = blocks[f][v, tile_rows(t - 1), :] if t else halos[f][v]
                put(stores[f], v, t, jnp.where(before, from_lo, jnp.where(after, from_hi, own)))

    def spread(ref, v, t):
        rows = tile_rows(t)
        here = ref[v, rows, :]
        at = SUB * (tiles if t == 0 else t) - 1
        total = ref[v, at : at + SUB, :] + ref[v, SUB * t + 1 : SUB * t + 1 + SUB, :]
        down = ref[(v - 1) % STRIDE, rows, :]
        up = ref[(v + 1) % STRIDE, rows, :]
        if v == 0:
            down = pltpu.roll(down, GROUP, 1)
        if v == STRIDE - 1:
            up = pltpu.roll(up, LANES - GROUP, 1)
        sides = pltpu.roll(here, 1, 1) + pltpu.roll(here, LANES - 1, 1)
        return total + (down + up) + sides, here

    def step(src, source, out):
        for v in range(STRIDE):
            for t in range(tiles):
                rows = tile_rows(t)
                total, here = spread(src, v, t)
                value = cs[v, rows, :] * total
                if source is not None:
                    value = source[v, rows, :] + value
                put(out, v, t, KEEP * here + value)

    step(hs, None, h1)
    step(bs, bs, y1)
    step(h1, None, h2)
    step(y1, bs, y2)
    its, ss = {}, {}
    for v in range(STRIDE):
        for t in range(1, tiles):
            rows = tile_rows(t)
            c, b = cs[v, rows, :], bs[v, rows, :]
            total_h, g2 = spread(h2, v, t)
            total_y, x3 = spread(y2, v, t)
            x2 = y1[v, rows, :]
            g1 = KEEP * g2 + c * total_h
            w3 = b + c * total_y
            it = KEEP * x3 + w3
            s = (g1 * b + g2 * (x2 - KEEP * b)) + (
                h1[v, rows, :] * (x3 - KEEP * x2) + hs[v, rows, :] * w3
            )
            its[v, t] = jnp.where(place < OWN, it, pltpu.roll(it, LANES - OWN, 1))
            ss[v, t] = jnp.where(place < OWN, s, pltpu.roll(s, LANES - OWN, 1))
    rim = (lane < DEPTH) | (lane >= LANES - DEPTH)
    copies = []
    for k in range(lz):
        z = level(k, lz)
        g, v = (k + DEPTH) // STRIDE, (k + DEPTH) % STRIDE
        shift = (LANES - DEPTH - (GROUP * g + DEPTH)) % LANES
        for t in range(1, tiles):
            block = tile_rows(t - 1)
            it = jnp.where(rim, pltpu.roll(its[v, t], shift, 1), it_in[k, block, :])
            s = jnp.where(rim, pltpu.roll(ss[v, t], shift, 1), s_in[k, block, :])
            it_out[k, block, :] = it + land_in[k, block, :]
            rg_out[k, block, :] = e_in[k, block, :] * s
        for i, (a, b) in enumerate(((it_out, it_hbm), (rg_out, rg_hbm))):
            copies.append(pltpu.make_async_copy(a.at[k], b.at[z], sem.at[i, k]))
            copies[-1].start()
    for copy in copies:
        copy.wait()


def body(nx, ny, log_range, sea_mask, forcing, cotangent):
    lz, lx, ly = forcing.shape
    f32 = jnp.float32
    sizes = (nx, ny, 2)
    vmem = pl.BlockSpec(memory_space=pltpu.VMEM)
    hbm = pl.BlockSpec(memory_space=pltpu.HBM)

    def call(kernel, shapes, args, name, scratch=(), flops=10**6, ins=vmem, outs=vmem):
        return pl.pallas_call(
            kernel,
            out_shape=[jax.ShapeDtypeStruct(s, f32) for s in shapes],
            in_specs=[ins] * len(args),
            out_specs=[outs] * len(shapes),
            scratch_shapes=[pltpu.VMEM(s, f32) if isinstance(s, tuple) else s for s in scratch],
            compiler_params=pltpu.CompilerParams(vmem_limit_bytes=16 * 2**20),
            cost_estimate=pl.CostEstimate(flops=flops, bytes_accessed=2**20, transcendentals=0),
            name=name,
        )(*args)

    block = (lz, lx, ly)
    store = (lz + DEPTH + 1, lx + 2 * SUB, ly)
    strip = (STRIDE, lx + 2 * SUB, LANES)
    slots = message_length(lx // SUB + 1)
    args = (log_range, sea_mask, forcing, cotangent)
    face = (DEPTH, lx, ly)
    (zmsg,) = call(
        prepare_z_kernel,
        [(3 * DEPTH - 1, lx, ly)],
        [pltpu.with_memory_space_constraint(a, pltpu.HBM) for a in args],
        "prepare_z",
        [face, pltpu.VMEM(face, jnp.int32), face, face, pltpu.SemaphoreType.DMA((4,))],
        ins=hbm,
    )
    c, b, h, e, land = call(prepare_kernel, [block] * 5, args, "prepare", flops=10**8)
    swap = [(d, d ^ 1) for d in range(2 * nx * ny)]
    zin = lax.ppermute(zmsg, AXES, swap)
    xa, xb = call(pack_x_kernel, [(lz + 1, SUB, ly)] * 2, (c, b, h, zin), "pack_x")
    xa = lax.ppermute(xa, AXES, pair_swaps(sizes, 0, 0))
    xb = lax.ppermute(xb, AXES, pair_swaps(sizes, 0, 1))
    pc, pb, ph, ya, yb = call(
        pack_block_kernel,
        [(STRIDE, lx, LANES)] * 3 + [(slots, SUB, LANES)] * 2,
        (c, b, h, zin),
        "pack_block",
        flops=10**8,
    )
    qc, qb, qh, yb, ya = call(
        functools.partial(pack_halo_kernel, nx, lz),
        [(STRIDE, SUB, LANES)] * 3 + [(slots, SUB, LANES)] * 2,
        (xa, xb, ya, yb),
        "pack_halo",
    )
    yb = lax.ppermute(yb, AXES, pair_swaps(sizes, 1, 1))
    ya = lax.ppermute(ya, AXES, pair_swaps(sizes, 1, 0))
    it, s = call(
        functools.partial(main_kernel, nx),
        [block] * 2,
        (c, b, h, zin, xa, xb),
        "main",
        [store] * 7,
        flops=2 * 10**8,
    )
    return call(
        functools.partial(edge_kernel, ny),
        [block] * 2,
        (pc, pb, ph, qc, qb, qh, yb, ya, it, s, e, land),
        "edge",
        [strip] * 7 + [block] * 2 + [pltpu.SemaphoreType.DMA((2, lz))],
        outs=hbm,
    )


def solution(mesh):
    nx, ny = mesh.shape["gx"], mesh.shape["gy"]
    spec = P("gz", "gx", "gy")
    return jax.shard_map(
        lambda *args: tuple(body(nx, ny, *args)),
        mesh=mesh,
        in_specs=(spec,) * 4,
        out_specs=(spec,) * 2,
        check_vma=False,
    )
```

```python
import functools

import jax
import jax.numpy as jnp
from jax import lax
from jax.experimental import pallas as pl
from jax.experimental.pallas import tpu as pltpu
from jax.sharding import PartitionSpec as P

SWEEPS = 4
RELAX = 0.9
KEEP = 1.0 - RELAX
SUB, LANES, DEPTH = 8, 128, SWEEPS - 1
OWN = 2 * DEPTH
GROUP = 2 * (OWN + DEPTH)
STRIDE = 3
AXES = ("gx", "gy", "gz")
ALL = slice(None)


def pair_swaps(sizes, axis, parity):
    nx, ny, nz = sizes
    pairs = []
    for i in range(nx):
        for j in range(ny):
            for k in range(nz):
                to = [i, j, k]
                other = to[axis] + (1 if to[axis] % 2 == parity else -1)
                if 0 <= other < sizes[axis]:
                    to[axis] = other
                else:
                    to[2] = 1 - k
                pairs.append(((i * ny + j) * nz + k, (to[0] * ny + to[1]) * nz + to[2]))
    return pairs


def iota(dim):
    return lax.broadcasted_iota(jnp.int32, (SUB, LANES), dim)


def level(t, lz):
    return jnp.where(lax.axis_index("gz") == 0, lz - 1 - t, t)


def tile_rows(t):
    return slice(SUB * t, SUB * (t + 1))


def coefficients(log_range, sea, source, cotangent):
    wet = sea != 0
    decay = jnp.exp(-2.0 * log_range)
    c = jnp.where(wet, RELAX / (6.0 + decay), 0.0)
    return wet, decay, c, c * source, c * cotangent


def prepare_z_kernel(lr_h, sea_h, src_h, cot_h, z_out, lr, sea, src, cot, sem):
    lz, lx = lr_h.shape[0], lr_h.shape[1]
    low = lax.axis_index("gz") == 0
    start = jnp.where(low, lz - DEPTH, 0)
    copies = [
        pltpu.make_async_copy(a.at[pl.ds(start, DEPTH)], b, sem.at[i])
        for i, (a, b) in enumerate(((lr_h, lr), (sea_h, sea), (src_h, src), (cot_h, cot)))
    ]
    for copy in copies:
        copy.start()
    for copy in copies:
        copy.wait()
    for t in range(DEPTH):
        z = jnp.where(low, DEPTH - 1 - t, t)
        for r in range(lx // SUB):
            rows = tile_rows(r)
            _, _, c, b, h = coefficients(
                lr[z, rows, :], sea[z, rows, :], src[z, rows, :], cot[z, rows, :]
            )
            z_out[t, rows, :] = b
            z_out[DEPTH + t, rows, :] = h
            if t < DEPTH - 1:
                z_out[2 * DEPTH + t, rows, :] = c


def prepare_kernel(lr, sea, src, cot, c_out, b_out, h_out, e_out, land_out):
    lz, lx, _ = lr.shape
    for t in range(lz):
        z = level(t, lz)
        for r in range(lx // SUB):
            rows = tile_rows(r)
            f = src[z, rows, :]
            wet, decay, c, b, h = coefficients(
                lr[z, rows, :], sea[z, rows, :], f, cot[z, rows, :]
            )
            c_out[t, rows, :] = c
            b_out[t, rows, :] = b
            h_out[t, rows, :] = h
            e_out[t, rows, :] = jnp.where(wet, (2.0 / RELAX) * decay, 0.0)
            land_out[t, rows, :] = jnp.where(
                wet, 0.0, RELAX * (1.0 + KEEP + KEEP**2 + KEEP**3) * f
            )


def local_or_z(local, zin, base, depth, z):
    if z >= DEPTH:
        return local, z - DEPTH
    t = DEPTH - 1 - z
    return (zin, base + t) if t < depth else (None, 0)


FACE = ((DEPTH, 0), (DEPTH, DEPTH), (DEPTH - 1, 2 * DEPTH))
CORNER = {1: ((2, 0), (2, 3), (1, 6)), 2: ((1, 2), (1, 5), (0, 0))}


def pack_x_kernel(c_in, b_in, h_in, zin, a_out, b_out):
    lz, lx, _ = c_in.shape
    odd = lax.axis_index("gx") % 2 == 1
    row = iota(0)
    for z in range(lz + 1):
        faces = []
        for rows, s in ((slice(0, SUB), 1), (slice(lx - SUB, lx), -1)):
            at = row if s == 1 else SUB - 1 - row
            if z < lz:
                parts = [(r[z, rows, :], q) for r, (_, q) in zip((b_in, h_in, c_in), FACE)]
            else:
                parts = [
                    (zin[DEPTH * f + t - 1, rows, :], CORNER[t][f][1])
                    for f in range(3)
                    for t in CORNER
                    if CORNER[t][f][0]
                ]
            parts.sort(key=lambda part: -part[1])
            face = None
            for tile, place in parts:
                if place:
                    tile = pltpu.roll(tile, (s * place) % SUB, 0)
                face = tile if face is None else jnp.where(at < limit, tile, face)
                limit = place
            faces.append(face)
        low, high = faces
        a_out[z] = jnp.where(odd, low, high)
        b_out[z] = jnp.where(odd, high, low)


def x_halo(a_in, b_in, z, index, size, row):
    zero = jnp.zeros((SUB, LANES), jnp.float32)
    if z >= DEPTH:
        at, fields = z - DEPTH, FACE
    else:
        at, fields = a_in.shape[0] - 1, CORNER.get(DEPTH - z)
    if fields is None:
        return zero, zero, zero
    odd = index % 2 == 1
    before = jnp.where(index > 0, jnp.where(odd, a_in[at], b_in[at]), zero)
    after = jnp.where(index < size - 1, jnp.where(odd, b_in[at], a_in[at]), zero)
    up = SUB - 1 - row

    def merge(depth, shift):
        if not depth:
            return zero
        lo = pltpu.roll(before, shift, 0) if shift else before
        hi = pltpu.roll(after, SUB - shift, 0) if shift else after
        return jnp.where(row < depth, hi, jnp.where(up < depth, lo, 0.0))

    return tuple(merge(*field) for field in fields)


def packed_place(lane, lz):
    group = lane // GROUP
    inside = group < -(-(lz + DEPTH) // STRIDE)
    return jnp.where(inside, group, -1), jnp.where(inside, lane - GROUP * group, -1)


BLOCK_FIELDS = ((1, DEPTH, 0), (2, DEPTH, DEPTH), (0, DEPTH, 2 * DEPTH))
HALO_FIELDS = ((1, DEPTH - 1, 0), (2, DEPTH - 1, DEPTH - 1), (0, DEPTH - 2, 2 * DEPTH - 2))


def message_slot(v, t, tiles):
    if t == 0:
        return 0, OWN * v
    if v < STRIDE - 1:
        return t, GROUP // 2 * v
    return tiles + (t - 1) // 2, GROUP // 2 * ((t - 1) % 2)


def message_length(tiles):
    return tiles + tiles // 2


def lane_roll(x, shift):
    return pltpu.roll(x, shift % LANES, 1) if shift % LANES else x


def pack_own(levels, first, count, tiles, place, group, sweep):
    zero = jnp.zeros((SUB, LANES), jnp.float32)
    raw = jnp.where(place < 2 * OWN, group, -1)
    acc = [[[zero] * count for _ in range(STRIDE)] for _ in range(3)]
    for z in range(levels):
        g, v = z // STRIDE, z % STRIDE
        for f in range(3):
            for t, tile in enumerate(sweep(f, z)):
                if tile is not None:
                    acc[f][v][t] = jnp.where(
                        raw == g, pltpu.roll(tile, (GROUP * g + OWN) % LANES, 1), acc[f][v][t]
                    )
    own = [[[None] * count for _ in range(STRIDE)] for _ in range(3)]
    sides = [{}, {}]
    for t in range(count):
        fields = BLOCK_FIELDS if first + t else HALO_FIELDS
        for v in range(STRIDE):
            slot, base = message_slot(v, first + t, tiles)
            for side in range(2):
                message = sides[side].get(slot)
                for f, depth, offset in fields:
                    at = OWN - depth if side == 0 else OWN
                    part = lane_roll(acc[f][v][t], base + offset - at)
                    if message is None:
                        message = part
                    else:
                        message = jnp.where(place >= base + offset, part, message)
                sides[side][slot] = message
            for f in range(3):
                a = acc[f][v][t]
                moved = pltpu.roll(a, GROUP - 2 * OWN, 1)
                own[f][v][t] = jnp.where(
                    place < OWN, a, jnp.where(place >= GROUP - OWN, moved, 0.0)
                )
    return own, sides


def put_messages(ya, yb, sides, odd):
    for slot in sides[0]:
        upper, lower = sides[0][slot], sides[1][slot]
        ya[slot] = jnp.where(odd, lower, upper)
        yb[slot] = jnp.where(odd, upper, lower)


def pack_block_kernel(c_in, b_in, h_in, zin, pc_out, pb_out, ph_out, ya, yb):
    lz, lx, _ = c_in.shape
    group, place = packed_place(iota(1), lz)
    odd = lax.axis_index("gy") % 2 == 1
    tiles = lx // SUB

    def sweep(f, z):
        ref, i = local_or_z(*(
            (c_in, zin, 2 * DEPTH, DEPTH - 1, z),
            (b_in, zin, 0, DEPTH, z),
            (h_in, zin, DEPTH, DEPTH, z),
        )[f])
        return [None if ref is None else ref[i, tile_rows(t), :] for t in range(tiles)]

    own, sides = pack_own(lz + DEPTH, 1, tiles, tiles + 1, place, group, sweep)
    put_messages(ya, yb, sides, odd)
    for t in range(tiles):
        for f, ref in enumerate((pc_out, pb_out, ph_out)):
            for v in range(STRIDE):
                ref[v, tile_rows(t), :] = own[f][v][t]


def pack_halo_kernel(nx, lz, xa, xb, ya_in, yb_in, pc_out, pb_out, ph_out, yb, ya):
    ix = lax.axis_index("gx")
    group, place = packed_place(iota(1), lz)
    odd = lax.axis_index("gy") % 2 == 1
    row = iota(0)
    parts = {}

    def sweep(f, z):
        if z not in parts:
            parts[z] = x_halo(xa, xb, z, ix, nx, row)
        return [parts[z][(f + 2) % 3]]

    own, sides = pack_own(lz + DEPTH, 0, 1, 0, place, group, sweep)
    put_messages(ya, yb, sides, odd)
    for src, dst in ((ya_in, ya), (yb_in, yb)):
        for i in range(1, src.shape[0]):
            dst[i] = src[i]
    for f, ref in enumerate((pc_out, pb_out, ph_out)):
        for v in range(STRIDE):
            ref[v] = own[f][v][0]


def main_kernel(nx, c_in, b_in, h_in, zin, xa, xb, it_out, s_out, cm, bm, hm, y1, y2, h1, h2):
    lz, lx, _ = it_out.shape
    tiles = lx // SUB + 1
    halo = tile_rows(tiles)
    zero = jnp.zeros((SUB, LANES), jnp.float32)
    ix, row = lax.axis_index("gx"), iota(0)
    for z in range(lz + DEPTH):
        parts = x_halo(xa, xb, z, ix, nx, row)
        local = (
            local_or_z(b_in, zin, 0, DEPTH, z),
            local_or_z(h_in, zin, DEPTH, DEPTH, z),
            local_or_z(c_in, zin, 2 * DEPTH, DEPTH - 1, z),
        )
        for f, store in enumerate((bm, hm, cm)):
            ref, i = local[f]
            for t in range(tiles):
                if t == 0:
                    tile = parts[f]
                    store[z, halo, :] = tile
                else:
                    tile = zero if ref is None else ref[i, tile_rows(t - 1), :]
                store[z, tile_rows(t), :] = tile
    for store in (cm, bm, hm):
        for t in range(tiles + 1):
            store[lz + DEPTH, tile_rows(t), :] = zero

    def spread(v, z, t):
        rows = tile_rows(t)
        here = v[z, rows, :]
        at = SUB * (tiles if t == 0 else t) - 1
        total = v[z, at : at + SUB, :] + v[z, SUB * t + 1 : SUB * t + 1 + SUB, :]
        total = total + (v[z - 1, rows, :] + v[z + 1, rows, :])
        sides = pltpu.roll(here, 1, 1) + pltpu.roll(here, LANES - 1, 1)
        return total + sides, here

    def step(v, source, out, start):
        for z in range(start, lz + DEPTH):
            for t in range(tiles):
                rows = tile_rows(t)
                total, here = spread(v, z, t)
                value = cm[z, rows, :] * total
                if source is not None:
                    value = source[z, rows, :] + value
                value = KEEP * here + value
                out[z, rows, :] = value
                if t == 0:
                    out[z, halo, :] = value
        for t in range(tiles + 1):
            out[lz + DEPTH, tile_rows(t), :] = zero

    step(hm, None, h1, 1)
    step(bm, bm, y1, 1)
    step(h1, None, h2, 2)
    step(y1, bm, y2, 2)
    for z in range(DEPTH, lz + DEPTH):
        for t in range(1, tiles):
            rows, block = tile_rows(t), tile_rows(t - 1)
            k = z - DEPTH
            c, b = cm[z, rows, :], bm[z, rows, :]
            total_h, g2 = spread(h2, z, t)
            total_y, x3 = spread(y2, z, t)
            x2 = y1[z, rows, :]
            g1 = KEEP * g2 + c * total_h
            w3 = b + c * total_y
            it_out[k, block, :] = KEEP * x3 + w3
            s_out[k, block, :] = (g1 * b + g2 * (x2 - KEEP * b)) + (
                h1[z, rows, :] * (x3 - KEEP * x2) + hm[z, rows, :] * w3
            )


def edge_kernel(ny, pc, pb, ph, qc, qb, qh, yb, ya, it_in, s_in, e_in, land_in, it_hbm, rg_hbm,
                cs, bs, hs, y1, y2, h1, h2, it_out, rg_out, sem):
    lz, lx, _ = e_in.shape
    iy = lax.axis_index("gy")
    lane = iota(1)
    group, place = packed_place(lane, lz)
    tiles = lx // SUB + 1
    halo = tile_rows(tiles)
    zero = jnp.zeros((SUB, LANES), jnp.float32)
    odd = iy % 2 == 1

    def put(ref, v, t, value):
        ref[v, tile_rows(t), :] = value
        if t == 0:
            ref[v, halo, :] = value

    slots = []
    for i in range(ya.shape[0]):
        a, b = ya[i], yb[i]
        slots.append(
            (
                jnp.where(iy > 0, jnp.where(odd, a, b), zero),
                jnp.where(iy < ny - 1, jnp.where(odd, b, a), zero),
            )
        )
    stores = (cs, bs, hs)
    blocks, halos = (pc, pb, ph), (qc, qb, qh)
    for t in range(tiles):
        for v in range(STRIDE):
            slot, base = message_slot(v, t, tiles)
            lo, hi = slots[slot]
            for f, depth, offset in BLOCK_FIELDS if t else HALO_FIELDS:
                end = OWN + 2 * DEPTH
                before = (place >= end - depth) & (place < end)
                after = (place >= OWN) & (place < OWN + depth)
                from_lo = lane_roll(lo, end - depth - base - offset)
                from_hi = lane_roll(hi, OWN - base - offset)
                own = blocks[f][v, tile_rows(t - 1), :] if t else halos[f][v]
                put(stores[f], v, t, jnp.where(before, from_lo, jnp.where(after, from_hi, own)))

    def spread(ref, v, t):
        rows = tile_rows(t)
        here = ref[v, rows, :]
        at = SUB * (tiles if t == 0 else t) - 1
        total = ref[v, at : at + SUB, :] + ref[v, SUB * t + 1 : SUB * t + 1 + SUB, :]
        down = ref[(v - 1) % STRIDE, rows, :]
        up = ref[(v + 1) % STRIDE, rows, :]
        if v == 0:
            down = pltpu.roll(down, GROUP, 1)
        if v == STRIDE - 1:
            up = pltpu.roll(up, LANES - GROUP, 1)
        sides = pltpu.roll(here, 1, 1) + pltpu.roll(here, LANES - 1, 1)
        return total + (down + up) + sides, here

    def advance(v, t, src, source, out):
        rows = tile_rows(t)
        total, here = spread(src, v, t)
        value = cs[v, rows, :] * total
        if source is not None:
            value = source[v, rows, :] + value
        put(out, v, t, KEEP * here + value)

    for chains in (((hs, None, h1), (bs, bs, y1)), ((h1, None, h2), (y1, bs, y2))):
        for t in range(tiles):
            for v in range(STRIDE):
                for chain in chains:
                    advance(v, t, *chain)
    rim = (lane < DEPTH) | (lane >= LANES - DEPTH)
    copies = []
    for t in range(1, tiles):
        rows, block = tile_rows(t), tile_rows(t - 1)
        its, ss = [], []
        for v in range(STRIDE):
            c, b = cs[v, rows, :], bs[v, rows, :]
            total_h, g2 = spread(h2, v, t)
            total_y, x3 = spread(y2, v, t)
            x2 = y1[v, rows, :]
            g1 = KEEP * g2 + c * total_h
            w3 = b + c * total_y
            it = KEEP * x3 + w3
            s = (g1 * b + g2 * (x2 - KEEP * b)) + (
                h1[v, rows, :] * (x3 - KEEP * x2) + hs[v, rows, :] * w3
            )
            its.append(jnp.where(place < OWN, it, pltpu.roll(it, LANES - OWN, 1)))
            ss.append(jnp.where(place < OWN, s, pltpu.roll(s, LANES - OWN, 1)))
        for k in range(lz):
            z = level(k, lz)
            g, v = (k + DEPTH) // STRIDE, (k + DEPTH) % STRIDE
            shift = (LANES - DEPTH - (GROUP * g + DEPTH)) % LANES
            it = jnp.where(rim, pltpu.roll(its[v], shift, 1), it_in[k, block, :])
            s = jnp.where(rim, pltpu.roll(ss[v], shift, 1), s_in[k, block, :])
            it_out[z, block, :] = it + land_in[k, block, :]
            rg_out[z, block, :] = e_in[k, block, :] * s
        for i, (a, b) in enumerate(((it_out, it_hbm), (rg_out, rg_hbm))):
            copies.append(
                pltpu.make_async_copy(a.at[:, block], b.at[:, block], sem.at[i, t - 1])
            )
            copies[-1].start()
    for copy in copies:
        copy.wait()


def body(nx, ny, log_range, sea_mask, forcing, cotangent):
    lz, lx, ly = forcing.shape
    f32 = jnp.float32
    sizes = (nx, ny, 2)
    vmem = pl.BlockSpec(memory_space=pltpu.VMEM)
    hbm = pl.BlockSpec(memory_space=pltpu.HBM)

    def call(kernel, shapes, args, name, scratch=(), flops=10**6, ins=vmem, outs=vmem):
        return pl.pallas_call(
            kernel,
            out_shape=[jax.ShapeDtypeStruct(s, f32) for s in shapes],
            in_specs=[ins] * len(args),
            out_specs=[outs] * len(shapes),
            scratch_shapes=[pltpu.VMEM(s, f32) if isinstance(s, tuple) else s for s in scratch],
            compiler_params=pltpu.CompilerParams(vmem_limit_bytes=16 * 2**20),
            cost_estimate=pl.CostEstimate(flops=flops, bytes_accessed=2**20, transcendentals=0),
            name=name,
        )(*args)

    block = (lz, lx, ly)
    store = (lz + DEPTH + 1, lx + 2 * SUB, ly)
    strip = (STRIDE, lx + 2 * SUB, LANES)
    slots = message_length(lx // SUB + 1)
    args = (log_range, sea_mask, forcing, cotangent)
    face = (DEPTH, lx, ly)
    (zmsg,) = call(
        prepare_z_kernel,
        [(3 * DEPTH - 1, lx, ly)],
        [pltpu.with_memory_space_constraint(a, pltpu.HBM) for a in args],
        "prepare_z",
        [face, pltpu.VMEM(face, jnp.int32), face, face, pltpu.SemaphoreType.DMA((4,))],
        ins=hbm,
    )
    c, b, h, e, land = call(prepare_kernel, [block] * 5, args, "prepare", flops=10**8)
    swap = [(d, d ^ 1) for d in range(2 * nx * ny)]
    zin = lax.ppermute(zmsg, AXES, swap)
    xa, xb = call(pack_x_kernel, [(lz + 1, SUB, ly)] * 2, (c, b, h, zin), "pack_x")
    xa = lax.ppermute(xa, AXES, pair_swaps(sizes, 0, 0))
    xb = lax.ppermute(xb, AXES, pair_swaps(sizes, 0, 1))
    pc, pb, ph, ya, yb = call(
        pack_block_kernel,
        [(STRIDE, lx, LANES)] * 3 + [(slots, SUB, LANES)] * 2,
        (c, b, h, zin),
        "pack_block",
        flops=10**8,
    )
    qc, qb, qh, yb, ya = call(
        functools.partial(pack_halo_kernel, nx, lz),
        [(STRIDE, SUB, LANES)] * 3 + [(slots, SUB, LANES)] * 2,
        (xa, xb, ya, yb),
        "pack_halo",
    )
    yb = lax.ppermute(yb, AXES, pair_swaps(sizes, 1, 1))
    ya = lax.ppermute(ya, AXES, pair_swaps(sizes, 1, 0))
    it, s = call(
        functools.partial(main_kernel, nx),
        [block] * 2,
        (c, b, h, zin, xa, xb),
        "main",
        [store] * 7,
        flops=2 * 10**8,
    )
    return call(
        functools.partial(edge_kernel, ny),
        [block] * 2,
        (pc, pb, ph, qc, qb, qh, yb, ya, it, s, e, land),
        "edge",
        [strip] * 7 + [block] * 2 + [pltpu.SemaphoreType.DMA((2, lx // SUB))],
        outs=hbm,
    )


def solution(mesh):
    nx, ny = mesh.shape["gx"], mesh.shape["gy"]
    spec = P("gz", "gx", "gy")
    return jax.shard_map(
        lambda *args: tuple(body(nx, ny, *args)),
        mesh=mesh,
        in_specs=(spec,) * 4,
        out_specs=(spec,) * 2,
        check_vma=False,
    )
```

```python
import functools

import jax
import jax.numpy as jnp
from jax import lax
from jax.experimental import pallas as pl
from jax.experimental.pallas import tpu as pltpu
from jax.sharding import PartitionSpec as P

SWEEPS = 4
RELAX = 0.9
KEEP = 1.0 - RELAX
SUB, LANES, DEPTH = 8, 128, SWEEPS - 1
OWN = 2 * DEPTH
GROUP = 2 * (OWN + DEPTH)
STRIDE = 3
AXES = ("gx", "gy", "gz")
ALL = slice(None)


def pair_swaps(sizes, axis, parity):
    nx, ny, nz = sizes
    pairs = []
    for i in range(nx):
        for j in range(ny):
            for k in range(nz):
                to = [i, j, k]
                other = to[axis] + (1 if to[axis] % 2 == parity else -1)
                if 0 <= other < sizes[axis]:
                    to[axis] = other
                else:
                    to[2] = 1 - k
                pairs.append(((i * ny + j) * nz + k, (to[0] * ny + to[1]) * nz + to[2]))
    return pairs


def iota(dim):
    return lax.broadcasted_iota(jnp.int32, (SUB, LANES), dim)


def level(t, lz):
    return jnp.where(lax.axis_index("gz") == 0, lz - 1 - t, t)


def tile_rows(t):
    return slice(SUB * t, SUB * (t + 1))


def coefficients(log_range, sea, source, cotangent):
    wet = sea != 0
    decay = jnp.exp(-2.0 * log_range)
    c = jnp.where(wet, RELAX / (6.0 + decay), 0.0)
    return wet, decay, c, c * source, c * cotangent


def prepare_z_kernel(lr_h, sea_h, src_h, cot_h, z_out, lr, sea, src, cot, sem):
    lz, lx = lr_h.shape[0], lr_h.shape[1]
    low = lax.axis_index("gz") == 0
    start = jnp.where(low, lz - DEPTH, 0)
    copies = [
        pltpu.make_async_copy(a.at[pl.ds(start, DEPTH)], b, sem.at[i])
        for i, (a, b) in enumerate(((lr_h, lr), (sea_h, sea), (src_h, src), (cot_h, cot)))
    ]
    for copy in copies:
        copy.start()
    for copy in copies:
        copy.wait()
    for t in range(DEPTH):
        z = jnp.where(low, DEPTH - 1 - t, t)
        for r in range(lx // SUB):
            rows = tile_rows(r)
            _, _, c, b, h = coefficients(
                lr[z, rows, :], sea[z, rows, :], src[z, rows, :], cot[z, rows, :]
            )
            z_out[t, rows, :] = b
            z_out[DEPTH + t, rows, :] = h
            if t < DEPTH - 1:
                z_out[2 * DEPTH + t, rows, :] = c


def prepare_kernel(lr, sea, src, cot, c_out, b_out, h_out, e_out, land_out):
    lz, lx, _ = lr.shape
    for t in range(lz):
        z = level(t, lz)
        for r in range(lx // SUB):
            rows = tile_rows(r)
            f = src[z, rows, :]
            wet, decay, c, b, h = coefficients(
                lr[z, rows, :], sea[z, rows, :], f, cot[z, rows, :]
            )
            c_out[t, rows, :] = c
            b_out[t, rows, :] = b
            h_out[t, rows, :] = h
            e_out[t, rows, :] = jnp.where(wet, (2.0 / RELAX) * decay, 0.0)
            land_out[t, rows, :] = jnp.where(
                wet, 0.0, RELAX * (1.0 + KEEP + KEEP**2 + KEEP**3) * f
            )


def local_or_z(local, zin, base, depth, z):
    if z >= DEPTH:
        return local, z - DEPTH
    t = DEPTH - 1 - z
    return (zin, base + t) if t < depth else (None, 0)


FACE = ((DEPTH, 0), (DEPTH, DEPTH), (DEPTH - 1, 2 * DEPTH))
CORNER = {1: ((2, 0), (2, 3), (1, 6)), 2: ((1, 2), (1, 5), (0, 0))}


def pack_x_kernel(c_in, b_in, h_in, zin, a_out, b_out):
    lz, lx, _ = c_in.shape
    odd = lax.axis_index("gx") % 2 == 1
    row = iota(0)
    for z in range(lz + 1):
        faces = []
        for rows, s in ((slice(0, SUB), 1), (slice(lx - SUB, lx), -1)):
            at = row if s == 1 else SUB - 1 - row
            if z < lz:
                parts = [(r[z, rows, :], q) for r, (_, q) in zip((b_in, h_in, c_in), FACE)]
            else:
                parts = [
                    (zin[DEPTH * f + t - 1, rows, :], CORNER[t][f][1])
                    for f in range(3)
                    for t in CORNER
                    if CORNER[t][f][0]
                ]
            parts.sort(key=lambda part: -part[1])
            face = None
            for tile, place in parts:
                if place:
                    tile = pltpu.roll(tile, (s * place) % SUB, 0)
                face = tile if face is None else jnp.where(at < limit, tile, face)
                limit = place
            faces.append(face)
        low, high = faces
        a_out[z] = jnp.where(odd, low, high)
        b_out[z] = jnp.where(odd, high, low)


def x_halo(a_in, b_in, z, index, size, row):
    zero = jnp.zeros((SUB, LANES), jnp.float32)
    if z >= DEPTH:
        at, fields = z - DEPTH, FACE
    else:
        at, fields = a_in.shape[0] - 1, CORNER.get(DEPTH - z)
    if fields is None:
        return zero, zero, zero
    odd = index % 2 == 1
    before = jnp.where(index > 0, jnp.where(odd, a_in[at], b_in[at]), zero)
    after = jnp.where(index < size - 1, jnp.where(odd, b_in[at], a_in[at]), zero)
    up = SUB - 1 - row

    def merge(depth, shift):
        if not depth:
            return zero
        lo = pltpu.roll(before, shift, 0) if shift else before
        hi = pltpu.roll(after, SUB - shift, 0) if shift else after
        return jnp.where(row < depth, hi, jnp.where(up < depth, lo, 0.0))

    return tuple(merge(*field) for field in fields)


def packed_place(lane, lz):
    group = lane // GROUP
    inside = group < -(-(lz + DEPTH) // STRIDE)
    return jnp.where(inside, group, -1), jnp.where(inside, lane - GROUP * group, -1)


def message_slot(v, t, tiles):
    if t == 0:
        depth = DEPTH - 1
        return 0, {
            1: (depth * v, depth),
            2: (depth * (STRIDE + v), depth),
            0: (2 * depth * STRIDE + v + 1, depth - 1),
        }
    if v < STRIDE - 1:
        slot, second = t, v
    else:
        slot, second = tiles + (t - 1) // 2, (t - 1) % 2
    return slot, {
        f: (2 * DEPTH * i + DEPTH * second, DEPTH) for i, f in enumerate((1, 2, 0))
    }


def message_length(tiles):
    return tiles + tiles // 2


def lane_roll(x, shift):
    return pltpu.roll(x, shift % LANES, 1) if shift % LANES else x


def window(first, depth):
    return first + depth - OWN


def packed_own(packed, start, place):
    return jnp.where(
        place < OWN, lane_roll(packed, -start),
        jnp.where(place >= GROUP - OWN, lane_roll(packed, OWN - start), 0.0),
    )


def pack_edges(levels, first, count, tiles, lane, place, sweep):
    zero = jnp.zeros((SUB, LANES), jnp.float32)
    groups = {}

    def group_from(start):
        if start not in groups:
            at = lane - start
            at = jnp.where(at < 0, at + LANES, jnp.where(at >= LANES, at - LANES, at))
            group = at // GROUP
            groups[start] = jnp.where(at - GROUP * group < 2 * OWN, group, -1)
        return groups[start]

    acc = {}
    for z in range(levels):
        g, v = z // STRIDE, z % STRIDE
        for f in range(3):
            for t, tile in enumerate(sweep(f, z)):
                start = window(*message_slot(v, first + t, tiles)[1][f])
                old = acc.get((f, v, t), zero)
                if tile is not None:
                    moved = lane_roll(tile, GROUP * g + start + OWN)
                    old = jnp.where(group_from(start) == g, moved, old)
                acc[f, v, t] = old
    parts = [{}, {}]
    for t in range(count):
        for v in range(STRIDE):
            slot, fields = message_slot(v, first + t, tiles)
            for f, (at, depth) in fields.items():
                for side in range(2):
                    begin = (at + side * depth) % GROUP
                    parts[side].setdefault(slot, []).append((begin, acc[f, v, t]))
    sides = [{}, {}]
    for side in range(2):
        for slot, pieces in parts[side].items():
            pieces.sort(key=lambda piece: piece[0])
            message = pieces[0][1]
            for begin, piece in pieces[1:]:
                message = jnp.where(place >= begin, piece, message)
            sides[side][slot] = message
    return acc, sides


def put_messages(ya, yb, sides, odd):
    for slot in sides[0]:
        upper, lower = sides[0][slot], sides[1][slot]
        ya[slot] = jnp.where(odd, lower, upper)
        yb[slot] = jnp.where(odd, upper, lower)


def pack_block_kernel(c_in, b_in, h_in, zin, pc_out, pb_out, ph_out, ya, yb):
    lz, lx, _ = c_in.shape
    lane = iota(1)
    _, place = packed_place(lane, lz)
    odd = lax.axis_index("gy") % 2 == 1
    tiles = lx // SUB

    def sweep(f, z):
        ref, i = local_or_z(*(
            (c_in, zin, 2 * DEPTH, DEPTH - 1, z),
            (b_in, zin, 0, DEPTH, z),
            (h_in, zin, DEPTH, DEPTH, z),
        )[f])
        return [None if ref is None else ref[i, tile_rows(t), :] for t in range(tiles)]

    packed, sides = pack_edges(lz + DEPTH, 1, tiles, tiles + 1, lane, place, sweep)
    put_messages(ya, yb, sides, odd)
    for t in range(tiles):
        for v in range(STRIDE):
            _, fields = message_slot(v, t + 1, tiles + 1)
            for f, ref in enumerate((pc_out, pb_out, ph_out)):
                ref[v, tile_rows(t), :] = packed_own(packed[f, v, t], window(*fields[f]), place)


def pack_halo_kernel(nx, lz, xa, xb, ya_in, yb_in, pc_out, pb_out, ph_out, yb, ya):
    ix = lax.axis_index("gx")
    lane = iota(1)
    _, place = packed_place(lane, lz)
    odd = lax.axis_index("gy") % 2 == 1
    row = iota(0)
    parts = {}

    def sweep(f, z):
        if z not in parts:
            parts[z] = x_halo(xa, xb, z, ix, nx, row)
        return [parts[z][(f + 2) % 3] if z >= (2, 1, 1)[f] else None]

    packed, sides = pack_edges(lz + DEPTH, 0, 1, 0, lane, place, sweep)
    put_messages(ya, yb, sides, odd)
    for src, dst in ((ya_in, ya), (yb_in, yb)):
        for i in range(1, src.shape[0]):
            dst[i] = src[i]
    for f, ref in enumerate((pc_out, pb_out, ph_out)):
        for v in range(STRIDE):
            ref[v] = packed[f, v, 0]


def main_kernel(nx, c_in, b_in, h_in, zin, xa, xb, uc, ub, uh, it_out, s_out, qc, qb, qh, cm, bm, hm, y1, y2, h1, h2):
    lz, lx, _ = it_out.shape
    tiles = lx // SUB + 1
    halo = tile_rows(tiles)
    zero = jnp.zeros((SUB, LANES), jnp.float32)
    ix, row = lax.axis_index("gx"), iota(0)
    _, place = packed_place(iota(1), lz)
    for v in range(STRIDE):
        _, fields = message_slot(v, 0, tiles)
        for f, (src, dst) in enumerate(((uc, qc), (ub, qb), (uh, qh))):
            dst[v] = packed_own(src[v], window(*fields[f]), place)
    for z in range(lz + DEPTH):
        parts = x_halo(xa, xb, z, ix, nx, row)
        local = (
            local_or_z(b_in, zin, 0, DEPTH, z),
            local_or_z(h_in, zin, DEPTH, DEPTH, z),
            local_or_z(c_in, zin, 2 * DEPTH, DEPTH - 1, z),
        )
        for f, store in enumerate((bm, hm, cm)):
            ref, i = local[f]
            for t in range(tiles):
                if t == 0:
                    tile = parts[f]
                    store[z, halo, :] = tile
                else:
                    tile = zero if ref is None else ref[i, tile_rows(t - 1), :]
                store[z, tile_rows(t), :] = tile
    for store in (cm, bm, hm):
        for t in range(tiles + 1):
            store[lz + DEPTH, tile_rows(t), :] = zero

    def spread(v, z, t):
        rows = tile_rows(t)
        here = v[z, rows, :]
        at = SUB * (tiles if t == 0 else t) - 1
        total = v[z, at : at + SUB, :] + v[z, SUB * t + 1 : SUB * t + 1 + SUB, :]
        total = total + (v[z - 1, rows, :] + v[z + 1, rows, :])
        sides = pltpu.roll(here, 1, 1) + pltpu.roll(here, LANES - 1, 1)
        return total + sides, here

    def step(v, source, out, start):
        for z in range(start, lz + DEPTH):
            for t in range(tiles):
                rows = tile_rows(t)
                total, here = spread(v, z, t)
                value = cm[z, rows, :] * total
                if source is not None:
                    value = source[z, rows, :] + value
                value = KEEP * here + value
                out[z, rows, :] = value
                if t == 0:
                    out[z, halo, :] = value
        for t in range(tiles + 1):
            out[lz + DEPTH, tile_rows(t), :] = zero

    step(hm, None, h1, 1)
    step(bm, bm, y1, 1)
    step(h1, None, h2, 2)
    step(y1, bm, y2, 2)
    for z in range(DEPTH, lz + DEPTH):
        for t in range(1, tiles):
            rows, block = tile_rows(t), tile_rows(t - 1)
            k = z - DEPTH
            c, b = cm[z, rows, :], bm[z, rows, :]
            total_h, g2 = spread(h2, z, t)
            total_y, x3 = spread(y2, z, t)
            x2 = y1[z, rows, :]
            g1 = KEEP * g2 + c * total_h
            w3 = b + c * total_y
            it_out[k, block, :] = KEEP * x3 + w3
            s_out[k, block, :] = (g1 * b + g2 * (x2 - KEEP * b)) + (
                h1[z, rows, :] * (x3 - KEEP * x2) + hm[z, rows, :] * w3
            )


def edge_kernel(ny, pc, pb, ph, qc, qb, qh, yb, ya, it_in, s_in, e_in, land_in, it_hbm, rg_hbm,
                cs, bs, hs, y1, y2, h1, h2, it_out, rg_out, sem):
    lz, lx, _ = e_in.shape
    iy = lax.axis_index("gy")
    lane = iota(1)
    group, place = packed_place(lane, lz)
    tiles = lx // SUB + 1
    halo = tile_rows(tiles)
    zero = jnp.zeros((SUB, LANES), jnp.float32)
    odd = iy % 2 == 1

    def put(ref, v, t, value):
        ref[v, tile_rows(t), :] = value
        if t == 0:
            ref[v, halo, :] = value

    slots = []
    for i in range(ya.shape[0]):
        a, b = ya[i], yb[i]
        slots.append(
            (
                jnp.where(iy > 0, jnp.where(odd, a, b), zero),
                jnp.where(iy < ny - 1, jnp.where(odd, b, a), zero),
            )
        )
    stores = (cs, bs, hs)
    blocks, halos = (pc, pb, ph), (qc, qb, qh)
    for t in range(tiles):
        for v in range(STRIDE):
            slot, fields = message_slot(v, t, tiles)
            lo, hi = slots[slot]
            for f, (first, depth) in fields.items():
                end = OWN + 2 * DEPTH
                before = (place >= end - depth) & (place < end)
                after = (place >= OWN) & (place < OWN + depth)
                from_lo = lane_roll(lo, end - depth - first)
                from_hi = lane_roll(hi, OWN - first - depth)
                own = blocks[f][v, tile_rows(t - 1), :] if t else halos[f][v]
                put(stores[f], v, t, jnp.where(before, from_lo, jnp.where(after, from_hi, own)))

    def spread(ref, v, t):
        rows = tile_rows(t)
        here = ref[v, rows, :]
        at = SUB * (tiles if t == 0 else t) - 1
        total = ref[v, at : at + SUB, :] + ref[v, SUB * t + 1 : SUB * t + 1 + SUB, :]
        down = ref[(v - 1) % STRIDE, rows, :]
        up = ref[(v + 1) % STRIDE, rows, :]
        if v == 0:
            down = pltpu.roll(down, GROUP, 1)
        if v == STRIDE - 1:
            up = pltpu.roll(up, LANES - GROUP, 1)
        sides = pltpu.roll(here, 1, 1) + pltpu.roll(here, LANES - 1, 1)
        return total + (down + up) + sides, here

    def advance(v, t, src, source, out):
        rows = tile_rows(t)
        total, here = spread(src, v, t)
        value = cs[v, rows, :] * total
        if source is not None:
            value = source[v, rows, :] + value
        put(out, v, t, KEEP * here + value)

    for chains in (((hs, None, h1), (bs, bs, y1)), ((h1, None, h2), (y1, bs, y2))):
        for t in range(tiles):
            for v in range(STRIDE):
                for chain in chains:
                    advance(v, t, *chain)
    rim = (lane < DEPTH) | (lane >= LANES - DEPTH)
    copies = []
    for t in range(1, tiles):
        rows, block = tile_rows(t), tile_rows(t - 1)
        its, ss = [], []
        for v in range(STRIDE):
            c, b = cs[v, rows, :], bs[v, rows, :]
            total_h, g2 = spread(h2, v, t)
            total_y, x3 = spread(y2, v, t)
            x2 = y1[v, rows, :]
            g1 = KEEP * g2 + c * total_h
            w3 = b + c * total_y
            it = KEEP * x3 + w3
            s = (g1 * b + g2 * (x2 - KEEP * b)) + (
                h1[v, rows, :] * (x3 - KEEP * x2) + hs[v, rows, :] * w3
            )
            its.append(jnp.where(place < OWN, it, pltpu.roll(it, LANES - OWN, 1)))
            ss.append(jnp.where(place < OWN, s, pltpu.roll(s, LANES - OWN, 1)))
        for k in range(lz):
            z = level(k, lz)
            g, v = (k + DEPTH) // STRIDE, (k + DEPTH) % STRIDE
            shift = (LANES - DEPTH - (GROUP * g + DEPTH)) % LANES
            it = jnp.where(rim, pltpu.roll(its[v], shift, 1), it_in[k, block, :])
            s = jnp.where(rim, pltpu.roll(ss[v], shift, 1), s_in[k, block, :])
            it_out[z, block, :] = it + land_in[k, block, :]
            rg_out[z, block, :] = e_in[k, block, :] * s
        for i, (a, b) in enumerate(((it_out, it_hbm), (rg_out, rg_hbm))):
            copies.append(
                pltpu.make_async_copy(a.at[:, block], b.at[:, block], sem.at[i, t - 1])
            )
            copies[-1].start()
    for copy in copies:
        copy.wait()


def body(nx, ny, log_range, sea_mask, forcing, cotangent):
    lz, lx, ly = forcing.shape
    f32 = jnp.float32
    sizes = (nx, ny, 2)
    vmem = pl.BlockSpec(memory_space=pltpu.VMEM)
    hbm = pl.BlockSpec(memory_space=pltpu.HBM)

    def call(kernel, shapes, args, name, scratch=(), flops=10**6, ins=vmem, outs=vmem):
        return pl.pallas_call(
            kernel,
            out_shape=[jax.ShapeDtypeStruct(s, f32) for s in shapes],
            in_specs=[ins] * len(args),
            out_specs=[outs] * len(shapes),
            scratch_shapes=[pltpu.VMEM(s, f32) if isinstance(s, tuple) else s for s in scratch],
            compiler_params=pltpu.CompilerParams(vmem_limit_bytes=16 * 2**20),
            cost_estimate=pl.CostEstimate(flops=flops, bytes_accessed=2**20, transcendentals=0),
            name=name,
        )(*args)

    block = (lz, lx, ly)
    store = (lz + DEPTH + 1, lx + 2 * SUB, ly)
    strip = (STRIDE, lx + 2 * SUB, LANES)
    slots = message_length(lx // SUB + 1)
    args = (log_range, sea_mask, forcing, cotangent)
    face = (DEPTH, lx, ly)
    (zmsg,) = call(
        prepare_z_kernel,
        [(3 * DEPTH - 1, lx, ly)],
        [pltpu.with_memory_space_constraint(a, pltpu.HBM) for a in args],
        "prepare_z",
        [face, pltpu.VMEM(face, jnp.int32), face, face, pltpu.SemaphoreType.DMA((4,))],
        ins=hbm,
    )
    c, b, h, e, land = call(prepare_kernel, [block] * 5, args, "prepare", flops=10**8)
    swap = [(d, d ^ 1) for d in range(2 * nx * ny)]
    zin = lax.ppermute(zmsg, AXES, swap)
    xa, xb = call(pack_x_kernel, [(lz + 1, SUB, ly)] * 2, (c, b, h, zin), "pack_x")
    xa = lax.ppermute(xa, AXES, pair_swaps(sizes, 0, 0))
    xb = lax.ppermute(xb, AXES, pair_swaps(sizes, 0, 1))
    pc, pb, ph, ya, yb = call(
        pack_block_kernel,
        [(STRIDE, lx, LANES)] * 3 + [(slots, SUB, LANES)] * 2,
        (c, b, h, zin),
        "pack_block",
        flops=10**8,
    )
    uc, ub, uh, yb, ya = call(
        functools.partial(pack_halo_kernel, nx, lz),
        [(STRIDE, SUB, LANES)] * 3 + [(slots, SUB, LANES)] * 2,
        (xa, xb, ya, yb),
        "pack_halo",
    )
    yb = lax.ppermute(yb, AXES, pair_swaps(sizes, 1, 1))
    ya = lax.ppermute(ya, AXES, pair_swaps(sizes, 1, 0))
    it, s, qc, qb, qh = call(
        functools.partial(main_kernel, nx),
        [block] * 2 + [(STRIDE, SUB, LANES)] * 3,
        (c, b, h, zin, xa, xb, uc, ub, uh),
        "main",
        [store] * 7,
        flops=2 * 10**8,
    )
    return call(
        functools.partial(edge_kernel, ny),
        [block] * 2,
        (pc, pb, ph, qc, qb, qh, yb, ya, it, s, e, land),
        "edge",
        [strip] * 7 + [block] * 2 + [pltpu.SemaphoreType.DMA((2, lx // SUB))],
        outs=hbm,
    )


def solution(mesh):
    nx, ny = mesh.shape["gx"], mesh.shape["gy"]
    spec = P("gz", "gx", "gy")
    return jax.shard_map(
        lambda *args: tuple(body(nx, ny, *args)),
        mesh=mesh,
        in_specs=(spec,) * 4,
        out_specs=(spec,) * 2,
        check_vma=False,
    )
```
